256 devices in a mesh: py: 32 (over z, x), px: 8 (over y, core).
Axes of the slice: x: 4, y: 4, z: 8, core: 2. Of those that a mesh axis runs over, the one named last changes fastest.
Arguments:
- density: float32 [1024, 256, 128], P('py', 'px'), may hold values from 0.5 to 2
- conductance: float32 [1024, 256, 128], P('py', 'px'), may hold values from 0.03 to 0.22
- source: float32 [1024, 256, 128], P('py', 'px'), may hold values from -0.2 to 0.2
Outputs:
- anomaly: float32 [1024, 256, 128], P('py', 'px')
- density_end: float32 [1024, 256, 128], P('py', 'px')
The draws below stay inside these ranges and needn't reach their ends.
All inputs are finite; a program needn't handle non-finite values.
Results may differ from the reference program's by a relative error of at most 0.00002.
Values sent between devices are 32-bit elements; how exact they have to be, the bound alone decides.
A program may use at most 64 MiB of HBM per device.

```python
import jax
import jax.numpy as jnp
from jax import lax

GRID_Y = 1024
GRID_X = 256
LEVELS = 128
STEPS = 6


def steps_of(rng, shape, cuts, least, high):
    loudness, own = 1.0, jax.random.fold_in(rng, 6)
    for dim, shards_of in cuts:
        steps = jnp.exp(jax.random.uniform(jax.random.fold_in(own, dim), (shards_of,), jnp.float32, least / len(cuts), high / len(cuts)))
        loudness = loudness * jnp.repeat(steps, shape[dim] // shards_of).reshape([-1 if axis == dim else 1 for axis in range(len(shape))])
    return loudness


def setup_inputs(seed: int = 0) -> dict:
    key_list = jax.random.split(jax.random.key(seed), 4)
    return {
        "density": jnp.clip(0.5 + 1.5 * jax.random.uniform(key_list[0], (GRID_Y, GRID_X, LEVELS), jnp.float32) ** steps_of(key_list[0], (GRID_Y, GRID_X, LEVELS), ((0, 32), (1, 8)), -0.2, 0.2), 0.5, 2.0),
        "conductance": jnp.clip(0.03 + 0.19 * jax.random.uniform(key_list[1], (GRID_Y, GRID_X, LEVELS), jnp.float32) ** steps_of(key_list[1], (GRID_Y, GRID_X, LEVELS), ((0, 32), (1, 8)), -0.2, 0.2), 0.03, 0.22),
        "source": jnp.clip(jax.random.uniform(key_list[2], (GRID_Y, GRID_X, LEVELS), jnp.float32, -0.2, 0.2) * steps_of(key_list[2], (GRID_Y, GRID_X, LEVELS), ((0, 32), (1, 8)), -0.4, 0.0), -0.2, 0.2),
    }


def strip_edges(values, dims):
    for dim in dims:
        values = lax.slice_in_dim(values, 1, values.shape[dim] - 1, axis=dim)
    return values

def neighbour(values, dim, start, dims):
    others = [other for other in dims if other != dim]
    values = strip_edges(values, others)
    return lax.slice_in_dim(values, start, start + values.shape[dim] - 2, axis=dim)

def one_step(padded, conductance, source):
    middle = strip_edges(padded, (0, 1))
    lower = [neighbour(padded, dim, 0, (0, 1)) for dim in (0, 1)]
    upper = [neighbour(padded, dim, 2, (0, 1)) for dim in (0, 1)]
    spread = lower[0] + upper[0] + lower[1] + upper[1] - 4.0 * middle
    return middle + conductance * spread + source

def reference(density, conductance, source):
    for step in range(STEPS):
        density = one_step(jnp.pad(density, ((1, 1), (1, 1), (0, 0)), mode='constant'), conductance, source)
    line_mean = lax.optimization_barrier(jnp.mean(density, axis=0, keepdims=True))
    centred = density - line_mean
    line_variance = lax.optimization_barrier(jnp.mean(centred * centred, axis=0, keepdims=True))
    anomaly = centred * lax.rsqrt(line_variance + 0.0001)
    return (anomaly, density)
```

```python
import functools

import jax
import jax.numpy as jnp
from jax import lax
from jax.experimental import pallas as pl
from jax.experimental.pallas import tpu as pltpu
from jax.sharding import PartitionSpec as P

STEPS = 6
EPS = 1e-4
XS = 4
ROWS, COLS, LEV = 32, 32, 128
TOP, LEFT = STEPS, 8
HIGH, WIDE = ROWS + 2 * STEPS, COLS + 2 * LEFT
MESH = pl.DeviceIdType.MESH
SIDES = [(a, b) for a in (-1, 0, 1) for b in (-1, 0, 1) if a or b]


def span(side, own, first, deep):
    if side == 0:
        return first, first, own
    if side > 0:
        return first + own - deep, first - deep, deep
    return first, first + own, deep


def piece(a, b, deep):
    deep_rows = deep_cols = deep
    if a and b:
        deep_rows = deep_cols = deep - 1
    rs, rd, rn = span(a, ROWS, TOP, deep_rows)
    cs, cd, cn = span(b, COLS, LEFT, deep_cols)
    return (pl.ds(rs, rn), pl.ds(cs, cn)), (pl.ds(rd, rn), pl.ds(cd, cn))


def merged(means, spreads, each):
    count = len(means)
    mean = sum(means[1:], means[0]) * (1.0 / count)
    spread = sum(spreads[1:], spreads[0])
    for m in means:
        spread = spread + each * (m - mean) * (m - mean)
    return mean, spread


def kernel(npy, npx, d_hbm, c_hbm, s_hbm, a_out, e_out, dt, cs, part, xin, zmine, zin,
           load_sem, hs_sem, hr_sem, xs_sem, xr_sem, zs_sem, zr_sem):
    py, px = lax.axis_index("py"), lax.axis_index("px")
    zs = npy // XS
    z, x = py // XS, lax.rem(py, XS)
    own = (pl.ds(TOP, ROWS), pl.ds(LEFT, COLS))
    loads = [
        pltpu.make_async_copy(d_hbm, dt.at[(0, *own)], load_sem.at[0]),
        pltpu.make_async_copy(c_hbm, cs.at[(0, *own)], load_sem.at[1]),
        pltpu.make_async_copy(s_hbm, cs.at[(1, *own)], load_sem.at[2]),
    ]
    for load in loads:
        load.start()

    def there(a, b):
        ok = None
        for side, at, count in ((a, py, npy), (b, px, npx)):
            if side:
                good = (at < count - 1) if side > 0 else (at > 0)
                ok = good if ok is None else ok & good
        return ok

    def xpeer(k):
        return {"py": z * XS + lax.rem(x + k, XS), "px": px}

    def zpeer(k):
        return {"py": lax.rem(z + k, zs) * XS + x, "px": px}

    barrier = pltpu.get_barrier_semaphore()
    for a, b in SIDES:
        @pl.when(there(a, b))
        def _():
            pl.semaphore_signal(barrier, inc=1, device_id={"py": py + a, "px": px + b}, device_id_type=MESH)
    for k in range(1, XS):
        pl.semaphore_signal(barrier, inc=1, device_id=xpeer(k), device_id_type=MESH)
    for k in range(1, zs):
        pl.semaphore_signal(barrier, inc=1, device_id=zpeer(k), device_id_type=MESH)

    for a in (-1, 1):
        @pl.when(jnp.logical_not(there(a, 0)))
        def _():
            rows = pl.ds(0, TOP) if a < 0 else pl.ds(TOP + ROWS, STEPS)
            dt[0, rows] = jnp.zeros((STEPS, WIDE, LEV), jnp.float32)
            cs[:, rows] = jnp.zeros((2, STEPS, WIDE, LEV), jnp.float32)
    for b in (-1, 1):
        @pl.when(jnp.logical_not(there(0, b)))
        def _():
            cols = pl.ds(0, LEFT) if b < 0 else pl.ds(LEFT + COLS, LEFT)
            dt[0, :, cols] = jnp.zeros((HIGH, LEFT, LEV), jnp.float32)
            cs[:, :, cols] = jnp.zeros((2, HIGH, LEFT, LEV), jnp.float32)

    for load in loads:
        load.wait()
    near = (py > 0).astype(jnp.int32) + (py < npy - 1).astype(jnp.int32)
    beside = (px > 0).astype(jnp.int32) + (px < npx - 1).astype(jnp.int32)
    pl.semaphore_wait(barrier, (near + 1) * (beside + 1) - 1 + XS - 1 + zs - 1)

    def halo(a, b):
        at = SIDES.index((a, b))
        (fr, fc), (tr, tc) = piece(a, b, STEPS)
        (gr, gc), (ur, uc) = piece(a, b, STEPS - 1)
        to = {"py": py + a, "px": px + b}
        return [
            pltpu.make_async_remote_copy(dt.at[0, fr, fc], dt.at[0, tr, tc], hs_sem.at[2 * at], hr_sem.at[2 * at], device_id=to, device_id_type=MESH),
            pltpu.make_async_remote_copy(cs.at[:, gr, gc], cs.at[:, ur, uc], hs_sem.at[2 * at + 1], hr_sem.at[2 * at + 1], device_id=to, device_id_type=MESH),
        ]

    order = [(a, b) for a, b in SIDES if a and b] + [(0, 1), (0, -1), (1, 0), (-1, 0)]
    for a, b in order:
        @pl.when(there(a, b))
        def _():
            for copy in halo(a, b):
                copy.start()

    def arrive(a, b):
        @pl.when(there(a, b))
        def _():
            for copy in halo(-a, -b):
                copy.wait_recv()

    def rows_of(step, low, count):
        @pl.loop(0, count)
        def _(i):
            r = low + i
            mid = dt[step, r]
            spread = dt[step, r - 1] + dt[step, r + 1] + (pltpu.roll(mid, 1, 0) + pltpu.roll(mid, WIDE - 1, 0)) - 4.0 * mid
            dt[step + 1, r] = mid + cs[0, r] * spread + cs[1, r]

    arrive(0, -1)
    arrive(0, 1)
    for step in range(STEPS):
        rows_of(step, TOP + step + 1, ROWS - 2 * (step + 1))
    block = pl.ds(LEFT, COLS)
    inner = ROWS - 2 * STEPS
    guess = lax.fori_loop(0, inner, lambda i, v: v + dt[STEPS, 2 * STEPS + i, block], jnp.zeros((COLS, LEV), jnp.float32)) * (1.0 / inner)

    def gather(low, count, totals):
        def add(i, totals):
            moved = dt[STEPS, low + i, block] - guess
            return totals[0] + moved, totals[1] + moved * moved
        return lax.fori_loop(0, count, add, totals)

    zero = jnp.zeros((COLS, LEV), jnp.float32)
    totals = gather(2 * STEPS, inner, (zero, zero))
    for a in (-1, 1):
        for b in (-1, 0, 1):
            arrive(a, b)
        for step in range(STEPS):
            low = step + 1 if a < 0 else TOP + ROWS - step - 1
            rows_of(step, low, STEPS)
        totals = gather(TOP if a < 0 else TOP + ROWS - STEPS, STEPS, totals)
    offset = totals[0] * (1.0 / ROWS)
    mean, spread = guess + offset, totals[1] - totals[0] * offset
    part[0] = mean
    part[1] = spread

    def over(peer, count, mine, got, send, recv, each):
        copies = []
        for k in range(1, count):
            copies.append(pltpu.make_async_remote_copy(mine, got.at[k - 1], send.at[k - 1], recv.at[k - 1], device_id=peer(k), device_id_type=MESH))
        for copy in copies:
            copy.start()
        for copy in copies:
            copy.wait_recv()
        means, spreads = [mine[0]] + [got[k, 0] for k in range(count - 1)], [mine[1]] + [got[k, 1] for k in range(count - 1)]
        return copies, *merged(means, spreads, each)

    sent, mean, spread = over(xpeer, XS, part, xin, xs_sem, xr_sem, float(ROWS))
    zmine[0] = mean
    zmine[1] = spread
    sent_z, mean, spread = over(zpeer, zs, zmine, zin, zs_sem, zr_sem, float(ROWS * XS))
    scale = lax.rsqrt(spread * (1.0 / (ROWS * npy)) + EPS)

    @pl.loop(0, ROWS)
    def _(i):
        value = dt[STEPS, TOP + i, block]
        e_out[i] = value
        a_out[i] = (value - mean) * scale

    for copy in sent + sent_z:
        copy.wait_send()
    for a, b in order:
        @pl.when(there(a, b))
        def _():
            for copy in halo(a, b):
                copy.wait_send()


def solution(mesh):
    npy, npx = mesh.shape["py"], mesh.shape["px"]
    zs = npy // XS

    def per_device(density, conductance, source):
        shape = jax.ShapeDtypeStruct((ROWS, COLS, LEV), jnp.float32)
        f32 = jnp.float32
        dma = pltpu.SemaphoreType.DMA
        return pl.pallas_call(
            functools.partial(kernel, npy, npx),
            name="diffuse",
            out_shape=(shape, shape),
            in_specs=[pl.BlockSpec(memory_space=pl.ANY)] * 3,
            out_specs=[pl.BlockSpec(memory_space=pltpu.VMEM)] * 2,
            scratch_shapes=[
                pltpu.VMEM((STEPS + 1, HIGH, WIDE, LEV), f32),
                pltpu.VMEM((2, HIGH, WIDE, LEV), f32),
                pltpu.VMEM((2, COLS, LEV), f32),
                pltpu.VMEM((XS - 1, 2, COLS, LEV), f32),
                pltpu.VMEM((2, COLS, LEV), f32),
                pltpu.VMEM((zs - 1, 2, COLS, LEV), f32),
                dma((3,)), dma((16,)), dma((16,)),
                dma((XS - 1,)), dma((XS - 1,)), dma((zs - 1,)), dma((zs - 1,)),
            ],
            compiler_params=pltpu.CompilerParams(collective_id=0, has_side_effects=True),
        )(density, conductance, source)

    spec = P("py", "px", None)
    return jax.shard_map(per_device, mesh=mesh, in_specs=(spec,) * 3, out_specs=(spec, spec), check_vma=False)
```

```python
import functools

import jax
import jax.numpy as jnp
from jax import lax
from jax.experimental import pallas as pl
from jax.experimental.pallas import tpu as pltpu
from jax.sharding import PartitionSpec as P

STEPS = 6
EPS = 1e-4
XS = 4
ROWS, COLS, LEV = 32, 32, 128
TOP, LEFT = STEPS, 8
HIGH, WIDE = ROWS + 2 * STEPS, COLS + 2 * LEFT
MESH = pl.DeviceIdType.MESH
SIDES = [(a, b) for a in (-1, 0, 1) for b in (-1, 0, 1) if a or b]


def span(side, own, first, deep):
    if side == 0:
        return first, first, own
    if side > 0:
        return first + own - deep, first - deep, deep
    return first, first + own, deep


def piece(a, b, deep):
    deep_rows = deep_cols = deep
    if a and b:
        deep_rows = deep_cols = deep - 1
    rs, rd, rn = span(a, ROWS, TOP, deep_rows)
    cs, cd, cn = span(b, COLS, LEFT, deep_cols)
    return (pl.ds(rs, rn), pl.ds(cs, cn)), (pl.ds(rd, rn), pl.ds(cd, cn))


def merged(means, spreads, each):
    count = len(means)
    mean = sum(means[1:], means[0]) * (1.0 / count)
    spread = sum(spreads[1:], spreads[0])
    for m in means:
        spread = spread + each * (m - mean) * (m - mean)
    return mean, spread


def kernel(npy, npx, d_hbm, c_hbm, s_hbm, e_out, stats, dt, cs, part, xin, zmine, zin,
           load_sem, hs_sem, hr_sem, xs_sem, xr_sem, zs_sem, zr_sem):
    py, px = lax.axis_index("py"), lax.axis_index("px")
    zs = npy // XS
    z, x = py // XS, lax.rem(py, XS)
    own = (pl.ds(TOP, ROWS), pl.ds(LEFT, COLS))
    loads = [
        pltpu.make_async_copy(d_hbm, dt.at[(0, *own)], load_sem.at[0]),
        pltpu.make_async_copy(c_hbm, cs.at[(0, *own)], load_sem.at[1]),
        pltpu.make_async_copy(s_hbm, cs.at[(1, *own)], load_sem.at[2]),
    ]
    for load in loads:
        load.start()

    def there(a, b):
        ok = None
        for side, at, count in ((a, py, npy), (b, px, npx)):
            if side:
                good = (at < count - 1) if side > 0 else (at > 0)
                ok = good if ok is None else ok & good
        return ok

    def xpeer(k):
        return {"py": z * XS + lax.rem(x + k, XS), "px": px}

    def zpeer(k):
        return {"py": lax.rem(z + k, zs) * XS + x, "px": px}

    barrier = pltpu.get_barrier_semaphore()
    for a, b in SIDES:
        @pl.when(there(a, b))
        def _():
            pl.semaphore_signal(barrier, inc=1, device_id={"py": py + a, "px": px + b}, device_id_type=MESH)
    for k in range(1, XS):
        pl.semaphore_signal(barrier, inc=1, device_id=xpeer(k), device_id_type=MESH)
    for k in range(1, zs):
        pl.semaphore_signal(barrier, inc=1, device_id=zpeer(k), device_id_type=MESH)

    for a in (-1, 1):
        @pl.when(jnp.logical_not(there(a, 0)))
        def _():
            rows = pl.ds(0, TOP) if a < 0 else pl.ds(TOP + ROWS, STEPS)
            dt[0, rows] = jnp.zeros((STEPS, WIDE, LEV), jnp.float32)
            cs[:, rows] = jnp.zeros((2, STEPS, WIDE, LEV), jnp.float32)
    for b in (-1, 1):
        @pl.when(jnp.logical_not(there(0, b)))
        def _():
            cols = pl.ds(0, LEFT) if b < 0 else pl.ds(LEFT + COLS, LEFT)
            dt[0, :, cols] = jnp.zeros((HIGH, LEFT, LEV), jnp.float32)
            cs[:, :, cols] = jnp.zeros((2, HIGH, LEFT, LEV), jnp.float32)

    with jax.named_scope("loads"):
        for load in loads:
            load.wait()
    near = (py > 0).astype(jnp.int32) + (py < npy - 1).astype(jnp.int32)
    beside = (px > 0).astype(jnp.int32) + (px < npx - 1).astype(jnp.int32)
    with jax.named_scope("barrier"):
        pl.semaphore_wait(barrier, (near + 1) * (beside + 1) - 1 + XS - 1 + zs - 1)

    def halo(a, b):
        at = SIDES.index((a, b))
        (fr, fc), (tr, tc) = piece(a, b, STEPS)
        (gr, gc), (ur, uc) = piece(a, b, STEPS - 1)
        to = {"py": py + a, "px": px + b}
        return [
            pltpu.make_async_remote_copy(dt.at[0, fr, fc], dt.at[0, tr, tc], hs_sem.at[2 * at], hr_sem.at[2 * at], device_id=to, device_id_type=MESH),
            pltpu.make_async_remote_copy(cs.at[:, gr, gc], cs.at[:, ur, uc], hs_sem.at[2 * at + 1], hr_sem.at[2 * at + 1], device_id=to, device_id_type=MESH),
        ]

    order = [(a, b) for a, b in SIDES if a and b] + [(0, 1), (0, -1), (1, 0), (-1, 0)]
    with jax.named_scope("sends"):
        for a, b in order:
            @pl.when(there(a, b))
            def _():
                for copy in halo(a, b):
                    copy.start()

    def arrive(a, b):
        @pl.when(there(a, b))
        def _():
            for copy in halo(-a, -b):
                copy.wait_recv()

    def rows_of(step, low, count):
        @pl.loop(0, count)
        def _(i):
            r = low + i
            mid = dt[step, r]
            spread = dt[step, r - 1] + dt[step, r + 1] + (pltpu.roll(mid, 1, 0) + pltpu.roll(mid, WIDE - 1, 0)) - 4.0 * mid
            dt[step + 1, r] = mid + cs[0, r] * spread + cs[1, r]

    with jax.named_scope("arrive_px"):
        arrive(0, -1)
        arrive(0, 1)
    with jax.named_scope("inner"):
        for step in range(STEPS):
            rows_of(step, TOP + step + 1, ROWS - 2 * (step + 1))
    block = pl.ds(LEFT, COLS)
    inner = ROWS - 2 * STEPS
    guess = lax.fori_loop(0, inner, lambda i, v: v + dt[STEPS, 2 * STEPS + i, block], jnp.zeros((COLS, LEV), jnp.float32)) * (1.0 / inner)

    def gather(low, count, totals):
        def add(i, totals):
            moved = dt[STEPS, low + i, block] - guess
            return totals[0] + moved, totals[1] + moved * moved
        return lax.fori_loop(0, count, add, totals)

    zero = jnp.zeros((COLS, LEV), jnp.float32)
    totals = gather(2 * STEPS, inner, (zero, zero))
    for a in (-1, 1):
        with jax.named_scope("arrive_py"):
            for b in (-1, 0, 1):
                arrive(a, b)
        with jax.named_scope("outer"):
            for step in range(STEPS):
                low = step + 1 if a < 0 else TOP + ROWS - step - 1
                rows_of(step, low, STEPS)
        totals = gather(TOP if a < 0 else TOP + ROWS - STEPS, STEPS, totals)
    offset = totals[0] * (1.0 / ROWS)
    mean, spread = guess + offset, totals[1] - totals[0] * offset
    part[0] = mean
    part[1] = spread

    def over(peer, count, mine, got, send, recv, each, meanwhile=None):
        copies = []
        for k in range(1, count):
            copies.append(pltpu.make_async_remote_copy(mine, got.at[k - 1], send.at[k - 1], recv.at[k - 1], device_id=peer(k), device_id_type=MESH))
        for copy in copies:
            copy.start()
        if meanwhile:
            meanwhile()
        for copy in copies:
            copy.wait_recv()
        means, spreads = [mine[0]] + [got[k, 0] for k in range(count - 1)], [mine[1]] + [got[k, 1] for k in range(count - 1)]
        return copies, *merged(means, spreads, each)

    def put_end():
        @pl.loop(0, ROWS)
        def _(i):
            e_out[i] = dt[STEPS, TOP + i, block]

    with jax.named_scope("over_x"):
        sent, mean, spread = over(xpeer, XS, part, xin, xs_sem, xr_sem, float(ROWS), put_end)
    zmine[0] = mean
    zmine[1] = spread
    with jax.named_scope("over_z"):
        sent_z, mean, spread = over(zpeer, zs, zmine, zin, zs_sem, zr_sem, float(ROWS * XS))
    scale = lax.rsqrt(spread * (1.0 / (ROWS * npy)) + EPS)

    stats[0] = mean
    stats[1] = scale
    for copy in sent + sent_z:
        copy.wait_send()
    for a, b in order:
        @pl.when(there(a, b))
        def _():
            for copy in halo(a, b):
                copy.wait_send()


def finish(end, stats, a_out, e_out, held, sem):
    whole = pltpu.make_async_copy(end, e_out, sem.at[0])
    whole.start()
    mean, scale = stats[0], stats[1]

    @pl.loop(0, ROWS)
    def _(i):
        held[i] = (end[i] - mean) * scale

    lines = pltpu.make_async_copy(held, a_out, sem.at[1])
    lines.start()
    whole.wait()
    lines.wait()


def solution(mesh):
    npy, npx = mesh.shape["py"], mesh.shape["px"]
    zs = npy // XS

    def per_device(density, conductance, source):
        shape = jax.ShapeDtypeStruct((ROWS, COLS, LEV), jnp.float32)
        f32 = jnp.float32
        dma = pltpu.SemaphoreType.DMA
        end, stats = pl.pallas_call(
            functools.partial(kernel, npy, npx),
            name="diffuse",
            out_shape=(pltpu.VMEM((ROWS, COLS, LEV), f32), pltpu.VMEM((2, COLS, LEV), f32)),
            in_specs=[pl.BlockSpec(memory_space=pl.ANY)] * 3,
            out_specs=[pl.BlockSpec(memory_space=pltpu.VMEM)] * 2,
            scratch_shapes=[
                pltpu.VMEM((STEPS + 1, HIGH, WIDE, LEV), f32),
                pltpu.VMEM((2, HIGH, WIDE, LEV), f32),
                pltpu.VMEM((2, COLS, LEV), f32),
                pltpu.VMEM((XS - 1, 2, COLS, LEV), f32),
                pltpu.VMEM((2, COLS, LEV), f32),
                pltpu.VMEM((zs - 1, 2, COLS, LEV), f32),
                dma((3,)), dma((16,)), dma((16,)),
                dma((XS - 1,)), dma((XS - 1,)), dma((zs - 1,)), dma((zs - 1,)),
            ],
            compiler_params=pltpu.CompilerParams(collective_id=0, has_side_effects=True),
        )(density, conductance, source)
        return pl.pallas_call(
            finish,
            name="finish",
            out_shape=(shape, shape),
            in_specs=[pl.BlockSpec(memory_space=pltpu.VMEM)] * 2,
            out_specs=[pl.BlockSpec(memory_space=pl.ANY)] * 2,
            scratch_shapes=[pltpu.VMEM((ROWS, COLS, LEV), f32), dma((2,))],
        )(*(pltpu.with_memory_space_constraint(v, pltpu.VMEM) for v in (end, stats)))

    spec = P("py", "px", None)
    return jax.shard_map(per_device, mesh=mesh, in_specs=(spec,) * 3, out_specs=(spec, spec), check_vma=False)
```

```python
import functools

import jax
import jax.numpy as jnp
from jax import lax
from jax.experimental import pallas as pl
from jax.experimental.pallas import tpu as pltpu
from jax.sharding import PartitionSpec as P

STEPS = 6
EPS = 1e-4
XS = 4
ROWS, COLS, LEV = 32, 32, 128
TOP, LEFT = STEPS, 8
HIGH, WIDE = ROWS + 2 * STEPS, COLS + 2 * LEFT
HALF = COLS // 2
MESH = pl.DeviceIdType.MESH
SIDES = [(a, b) for a in (-1, 0, 1) for b in (-1, 0, 1) if a or b]
GROUPS = (((1, 3), (1, 2)), ((4, 5), (3, 4)), ((6, 6), (5, 5)))
DIAGONALS = ((1, 2, 3), (4, 5), (6,))
CORNER_D = ((1, 2, 5), (3, 5, 3))
CORNER_CS = ((1, 2, 4), (3, 4, 2))


def reach(side, size, start, first, last):
    length = last - first + 1
    if side > 0:
        return pl.ds(start + size - last, length), pl.ds(start - last, length)
    return pl.ds(start + first - 1, length), pl.ds(start + size + first - 1, length)


def halo_pieces(a, b):
    rows, cols = pl.ds(TOP, ROWS), pl.ds(LEFT, COLS)
    out = []
    if a and b:
        for which, pieces in ((0, CORNER_D), (1, CORNER_CS)):
            for first, last, wide in pieces:
                (fr, tr), (fc, tc) = reach(a, ROWS, TOP, first, last), reach(b, COLS, LEFT, 1, wide)
                out.append((which, (fr, fc), (tr, tc)))
    elif b:
        for which, deep in ((0, STEPS), (1, STEPS - 1)):
            fc, tc = reach(b, COLS, LEFT, 1, deep)
            out.append((which, (rows, fc), (rows, tc)))
    else:
        for group in GROUPS:
            for which, (first, last) in enumerate(group):
                fr, tr = reach(a, ROWS, TOP, first, last)
                out.append((which, (fr, cols), (tr, cols)))
    return out


PIECES = {side: halo_pieces(*side) for side in SIDES}
FIRST = {}
for _side in SIDES:
    FIRST[_side] = sum(len(PIECES[s]) for s in FIRST)
COPIES = sum(len(p) for p in PIECES.values())


def merged(means, spreads, each):
    mean = sum(means[1:], means[0]) * (1.0 / len(means))
    spread = sum(spreads[1:], spreads[0])
    for m in means:
        spread = spread + each * (m - mean) * (m - mean)
    return mean, spread


def kernel(npy, npx, d_hbm, c_hbm, s_hbm, e_out, stats, dt, cs, part, mid_part, xin, zin,
           load_sem, hs_sem, hr_sem, xs_sem, xr_sem, zs_sem, zr_sem):
    py, px = lax.axis_index("py"), lax.axis_index("px")
    zs = npy // XS
    z, x = py // XS, lax.rem(py, XS)
    own = (pl.ds(TOP, ROWS), pl.ds(LEFT, COLS))
    loads = [
        pltpu.make_async_copy(d_hbm, dt.at[(0, *own)], load_sem.at[0]),
        pltpu.make_async_copy(c_hbm, cs.at[(0, *own)], load_sem.at[1]),
        pltpu.make_async_copy(s_hbm, cs.at[(1, *own)], load_sem.at[2]),
    ]
    for load in loads:
        load.start()

    def there(a, b):
        ok = None
        for side, at, count in ((a, py, npy), (b, px, npx)):
            if side:
                good = (at < count - 1) if side > 0 else (at > 0)
                ok = good if ok is None else ok & good
        return ok

    def xpeer(k):
        return {"py": z * XS + lax.rem(x + k, XS), "px": px}

    def zpeer(k):
        return {"py": lax.rem(z + k, zs) * XS + x, "px": px}

    barrier = pltpu.get_barrier_semaphore()
    for a, b in SIDES:
        @pl.when(there(a, b))
        def _():
            pl.semaphore_signal(barrier, inc=1, device_id={"py": py + a, "px": px + b}, device_id_type=MESH)
    for k in range(1, XS):
        pl.semaphore_signal(barrier, inc=1, device_id=xpeer(k), device_id_type=MESH)
    for k in range(1, zs):
        pl.semaphore_signal(barrier, inc=1, device_id=zpeer(k), device_id_type=MESH)

    for a in (-1, 1):
        @pl.when(jnp.logical_not(there(a, 0)))
        def _():
            rows = pl.ds(0, TOP) if a < 0 else pl.ds(TOP + ROWS, STEPS)
            dt[0, rows] = jnp.zeros((STEPS, WIDE, LEV), jnp.float32)
            cs[:, rows] = jnp.zeros((2, STEPS, WIDE, LEV), jnp.float32)
    for b in (-1, 1):
        @pl.when(jnp.logical_not(there(0, b)))
        def _():
            cols = pl.ds(0, LEFT) if b < 0 else pl.ds(LEFT + COLS, LEFT)
            dt[0, :, cols] = jnp.zeros((HIGH, LEFT, LEV), jnp.float32)
            cs[:, :, cols] = jnp.zeros((2, HIGH, LEFT, LEV), jnp.float32)

    with jax.named_scope("loads"):
        for load in loads:
            load.wait()
    near = (py > 0).astype(jnp.int32) + (py < npy - 1).astype(jnp.int32)
    beside = (px > 0).astype(jnp.int32) + (px < npx - 1).astype(jnp.int32)
    with jax.named_scope("barrier"):
        pl.semaphore_wait(barrier, (near + 1) * (beside + 1) - 1 + XS - 1 + zs - 1)

    def halo(a, b, part=slice(None)):
        to = {"py": py + a, "px": px + b}
        copies = []
        for at, (which, source, target) in list(enumerate(PIECES[a, b], FIRST[a, b]))[part]:
            if which:
                src, dst = cs.at[(slice(None), *source)], cs.at[(slice(None), *target)]
            else:
                src, dst = dt.at[(0, *source)], dt.at[(0, *target)]
            copies.append(pltpu.make_async_remote_copy(src, dst, hs_sem.at[at], hr_sem.at[at], device_id=to, device_id_type=MESH))
        return copies

    order = [(0, 1), (0, -1)] + [(a, b) for a, b in SIDES if a and b] + [(1, 0), (-1, 0)]
    with jax.named_scope("sends"):
        for a, b in order:
            @pl.when(there(a, b))
            def _():
                for copy in halo(a, b):
                    copy.start()

    def arrive(a, b, part=slice(None)):
        @pl.when(there(a, b))
        def _():
            for copy in halo(-a, -b, part):
                copy.wait_recv()

    def later(above, mid, below, r):
        spread = (above + below) + (pltpu.roll(mid, 1, 0) + pltpu.roll(mid, WIDE - 1, 0)) - 4.0 * mid
        return mid + cs[0, r] * spread + cs[1, r]

    with jax.named_scope("arrive_px"):
        arrive(0, -1)
        arrive(0, 1)
    with jax.named_scope("inner"):
        for step in range(STEPS):
            low, count = TOP + step + 1, ROWS - 2 * (step + 1)

            @pl.loop(0, count // 2)
            def _(i):
                r = low + 2 * i
                lines = [dt[step, r + n] for n in range(-1, 3)]
                dt[step + 1, r] = later(*lines[:3], r)
                dt[step + 1, r + 1] = later(*lines[1:], r + 1)

    block = pl.ds(LEFT, COLS)
    inner = ROWS - 2 * STEPS
    zero = jnp.zeros((COLS, LEV), jnp.float32)
    with jax.named_scope("gather"):
        guess = lax.fori_loop(0, inner // 4, lambda i, v: v + sum(dt[STEPS, 2 * STEPS + 4 * i + n, block] for n in range(4)), zero) * (1.0 / inner)

        def gather(lines, totals):
            for line in lines:
                moved = line - guess
                totals = (totals[0] + moved, totals[1] + moved * moved)
            return totals

        totals = lax.fori_loop(0, inner // 2, lambda i, t: gather([dt[STEPS, 2 * STEPS + 2 * i + n, block] for n in range(2)], t), (zero, zero))

    for n, diagonals in enumerate(DIAGONALS):
        with jax.named_scope("arrive_py"):
            for a in (-1, 1):
                if n == 0:
                    for b in (-1, 1):
                        arrive(a, b)
                arrive(a, 0, slice(2 * n, 2 * n + 2))
        with jax.named_scope("outer"):
            for k in diagonals:
                up = dt[0, TOP - k]
                down = dt[0, TOP + ROWS - 1 + k]
                for t in range(STEPS):
                    r, q = TOP - k + t + 1, TOP + ROWS - 2 + k - t
                    up = later(up, dt[t, r], dt[t, r + 1], r)
                    down = later(dt[t, q - 1], dt[t, q], down, q)
                    dt[t + 1, r] = up
                    dt[t + 1, q] = down
    with jax.named_scope("part"):
        totals = gather([dt[STEPS, r, block] for n in range(STEPS) for r in (TOP + n, TOP + ROWS - 1 - n)], totals)
        offset = totals[0] * (1.0 / ROWS)
        part[0] = guess + offset
        part[1] = totals[1] - totals[0] * offset

    def send(peer, count, mine, got, sends, recvs, at):
        base = at * (count - 1)
        return [
            pltpu.make_async_remote_copy(mine, got.at[base + k - 1], sends.at[base + k - 1], recvs.at[base + k - 1], device_id=peer(k), device_id_type=MESH)
            for k in range(1, count)
        ]

    def start(copies):
        middle = len(copies) // 2
        for k in sorted(range(len(copies)), key=lambda k: abs(k - middle)):
            copies[k].start()

    def collect(copies, mine, got, at, each):
        for copy in copies:
            copy.wait_recv()
        base = at * len(copies)
        return merged(*([mine[s]] + [got[base + k, s] for k in range(len(copies))] for s in (0, 1)), each)

    halves = [part.at[:, pl.ds(h * HALF, HALF)] for h in (0, 1)]
    cells = float(ROWS)
    xa = send(xpeer, XS, halves[0], xin, xs_sem, xr_sem, 0)
    zb = send(zpeer, zs, halves[1], zin, zs_sem, zr_sem, 1)
    za = send(zpeer, zs, mid_part.at[0], zin, zs_sem, zr_sem, 0)
    xb = send(xpeer, XS, mid_part.at[1], xin, xs_sem, xr_sem, 1)
    start(xa)
    start(zb)

    @pl.loop(0, ROWS)
    def _(i):
        e_out[i] = dt[STEPS, TOP + i, block]

    with jax.named_scope("xa"):
        mid_part[0, 0], mid_part[0, 1] = collect(xa, halves[0], xin, 0, cells)
    start(za)
    with jax.named_scope("zb"):
        mid_part[1, 0], mid_part[1, 1] = collect(zb, halves[1], zin, 1, cells)
    start(xb)
    with jax.named_scope("za"):
        mean_a, spread_a = collect(za, mid_part.at[0], zin, 0, cells * XS)
        stats[0, :HALF] = mean_a
        stats[1, :HALF] = lax.rsqrt(spread_a * (1.0 / (ROWS * npy)) + EPS)
    with jax.named_scope("xb"):
        mean_b, spread_b = collect(xb, mid_part.at[1], xin, 1, cells * zs)
        stats[0, HALF:] = mean_b
        stats[1, HALF:] = lax.rsqrt(spread_b * (1.0 / (ROWS * npy)) + EPS)
    for copy in xa + xb + za + zb:
        copy.wait_send()
    for a, b in order:
        @pl.when(there(a, b))
        def _():
            for copy in halo(a, b):
                copy.wait_send()


def finish(end, stats, a_out, e_out, held, sem):
    whole = pltpu.make_async_copy(end, e_out, sem.at[0])
    whole.start()
    mean, scale = stats[0], stats[1]
    quarter = ROWS // 4
    copies = []
    for q in range(4):
        @pl.loop(q * quarter, (q + 1) * quarter)
        def _(i):
            held[i] = (end[i] - mean) * scale

        rows = pl.ds(q * quarter, quarter)
        copies.append(pltpu.make_async_copy(held.at[rows], a_out.at[rows], sem.at[1 + q]))
        copies[-1].start()
    whole.wait()
    for copy in copies:
        copy.wait()


def solution(mesh):
    npy, npx = mesh.shape["py"], mesh.shape["px"]
    zs = npy // XS

    def per_device(density, conductance, source):
        shape = jax.ShapeDtypeStruct((ROWS, COLS, LEV), jnp.float32)
        f32 = jnp.float32
        dma = pltpu.SemaphoreType.DMA
        end, stats = pl.pallas_call(
            functools.partial(kernel, npy, npx),
            name="diffuse",
            out_shape=(pltpu.VMEM((ROWS, COLS, LEV), f32), pltpu.VMEM((2, COLS, LEV), f32)),
            in_specs=[pl.BlockSpec(memory_space=pl.ANY)] * 3,
            out_specs=[pl.BlockSpec(memory_space=pltpu.VMEM)] * 2,
            scratch_shapes=[
                pltpu.VMEM((STEPS + 1, HIGH, WIDE, LEV), f32),
                pltpu.VMEM((2, HIGH, WIDE, LEV), f32),
                pltpu.VMEM((2, COLS, LEV), f32),
                pltpu.VMEM((2, 2, HALF, LEV), f32),
                pltpu.VMEM((2 * (XS - 1), 2, HALF, LEV), f32),
                pltpu.VMEM((2 * (zs - 1), 2, HALF, LEV), f32),
                dma((3,)), dma((COPIES,)), dma((COPIES,)),
                dma((2 * (XS - 1),)), dma((2 * (XS - 1),)), dma((2 * (zs - 1),)), dma((2 * (zs - 1),)),
            ],
            compiler_params=pltpu.CompilerParams(collective_id=0, has_side_effects=True),
        )(density, conductance, source)
        return pl.pallas_call(
            finish,
            name="finish",
            out_shape=(shape, shape),
            in_specs=[pl.BlockSpec(memory_space=pltpu.VMEM)] * 2,
            out_specs=[pl.BlockSpec(memory_space=pl.ANY)] * 2,
            scratch_shapes=[pltpu.VMEM((ROWS, COLS, LEV), f32), dma((5,))],
        )(*(pltpu.with_memory_space_constraint(v, pltpu.VMEM) for v in (end, stats)))

    spec = P("py", "px", None)
    return jax.shard_map(per_device, mesh=mesh, in_specs=(spec,) * 3, out_specs=(spec, spec), check_vma=False)
```

```python
import functools

import jax
import jax.numpy as jnp
from jax import lax
from jax.experimental import pallas as pl
from jax.experimental.pallas import tpu as pltpu
from jax.sharding import PartitionSpec as P

STEPS = 6
EPS = 1e-4
XS = 4
ROWS, COLS, LEV = 32, 32, 128
TOP, LEFT = STEPS, 8
HIGH, WIDE = ROWS + 2 * STEPS, COLS + 2 * LEFT
HALF = COLS // 2
MESH = pl.DeviceIdType.MESH
SIDES = [(a, b) for a in (-1, 0, 1) for b in (-1, 0, 1) if a or b]
SKY, LATE = 4, 2
FIELD, COEF, AHEAD = 0, 1, 2
DIAGONALS = ((1, 2, 3), (4,), (5, 6))


def reach(side, size, start, first, last):
    length = last - first + 1
    if side > 0:
        return pl.ds(start + size - last, length), pl.ds(start - last, length)
    return pl.ds(start + first - 1, length), pl.ds(start + size + first - 1, length)


def halo_groups(a, b):
    def to(which, rows, cols):
        (fr, tr), (fc, tc) = rows, cols
        return which, (fr, fc), (tr, tc), fr.size * fc.size * (2 if which == COEF else 1)

    def rows_of(first, last):
        return reach(a, ROWS, TOP, first, last)

    def cols_of(first, last):
        return reach(b, COLS, LEFT, first, last)

    def same(start, size):
        return pl.ds(start, size), pl.ds(start, size)

    whole = same(LEFT, COLS)
    if a and b:
        return [[
            to(FIELD, rows_of(1, 2), cols_of(1, 5)), to(FIELD, rows_of(3, 5), cols_of(1, 3)),
            to(COEF, rows_of(1, 2), cols_of(1, 4)), to(COEF, rows_of(3, 4), cols_of(1, 2)),
        ]]
    if b:
        return [[to(FIELD, same(TOP, ROWS), cols_of(1, STEPS)), to(COEF, same(TOP, ROWS), cols_of(1, STEPS - 1))]]
    edges = []
    for left in (True, False):
        edges.append(to(FIELD, rows_of(5, 6), same(LEFT if left else LEFT + COLS - 3, 3)))
        edges.append(to(COEF, rows_of(4, 5), same(LEFT if left else LEFT + COLS - 2, 2)))
    side = same(0, LATE)
    return [
        [to(FIELD, rows_of(1, 3), whole), to(COEF, rows_of(1, 2), whole)],
        [to(FIELD, rows_of(4, 4), whole), to(COEF, rows_of(3, 3), whole)],
        edges + [to(AHEAD, side, same(0, COLS))],
    ]


GROUPS = {side: halo_groups(*side) for side in SIDES}
BASE = {}
for _side in SIDES:
    BASE[_side] = sum(len(GROUPS[s]) for s in BASE)
COPIES = sum(len(g) for g in GROUPS.values())


def area(cells):
    for rows in range(1, HIGH + 1):
        if cells % rows == 0 and cells // rows <= WIDE:
            return pl.ds(0, rows), pl.ds(0, cells // rows)
    raise ValueError(cells)


def merged(means, spreads, each):
    mean = sum(means[1:], means[0]) * (1.0 / len(means))
    spread = sum(spreads[1:], spreads[0])
    for m in means:
        spread = spread + each * (m - mean) * (m - mean)
    return mean, spread


def kernel(npy, npx, d_hbm, c_hbm, s_hbm, e_out, stats, dt, cs, sky, ahead, part, mid_part, xin, zin,
           load_sem, hs_sem, hr_sem, ts_sem, tr_sem, token):
    py, px = lax.axis_index("py"), lax.axis_index("px")
    zs = npy // XS
    z, x = py // XS, lax.rem(py, XS)
    rounds = 0
    while 2 ** rounds < zs // 2:
        rounds += 1
    own = (pl.ds(TOP, ROWS), pl.ds(LEFT, COLS))

    def there(a, b):
        ok = None
        for side, at, count in ((a, py, npy), (b, px, npx)):
            if side:
                good = (at < count - 1) if side > 0 else (at > 0)
                ok = good if ok is None else ok & good
        return ok

    def xpeer(k):
        return {"py": z * XS + lax.rem(x + k, XS), "px": px}

    def zpeer(k):
        return {"py": lax.rem(z + k, zs) * XS + x, "px": px}

    barrier = pltpu.get_barrier_semaphore()
    for a, b in SIDES:
        @pl.when(there(a, b))
        def _():
            pl.semaphore_signal(barrier, inc=1, device_id={"py": py + a, "px": px + b}, device_id_type=MESH)
    for k in range(1, XS):
        pl.semaphore_signal(barrier, inc=1, device_id=xpeer(k), device_id_type=MESH)
    beyond = sorted({1, zs - 1})
    for k in beyond:
        pl.semaphore_signal(barrier, inc=1, device_id=zpeer(k), device_id_type=MESH)

    loads = [
        pltpu.make_async_copy(d_hbm, dt.at[(0, *own)], load_sem.at[0]),
        pltpu.make_async_copy(c_hbm, cs.at[(0, *own)], load_sem.at[1]),
        pltpu.make_async_copy(s_hbm, cs.at[(1, *own)], load_sem.at[2]),
    ]
    for load in loads:
        load.start()

    for a in (-1, 1):
        @pl.when(jnp.logical_not(there(a, 0)))
        def _():
            rows = pl.ds(0, TOP) if a < 0 else pl.ds(TOP + ROWS, STEPS)
            dt[0, rows] = jnp.zeros((STEPS, WIDE, LEV), jnp.float32)
            cs[:, rows] = jnp.zeros((2, STEPS, WIDE, LEV), jnp.float32)
            sky[(a + 1) // 2] = jnp.zeros((LATE, COLS, LEV), jnp.float32)
    for b in (-1, 1):
        @pl.when(jnp.logical_not(there(0, b)))
        def _():
            cols = pl.ds(0, LEFT) if b < 0 else pl.ds(LEFT + COLS, LEFT)
            dt[0, :, cols] = jnp.zeros((HIGH, LEFT, LEV), jnp.float32)
            cs[:, :, cols] = jnp.zeros((2, HIGH, LEFT, LEV), jnp.float32)

    with jax.named_scope("loads"):
        for load in loads:
            load.wait()
    block = pl.ds(LEFT, COLS)

    def later(above, mid, below, r, cols=slice(None)):
        width = mid.shape[0]
        spread = (above + below) + (pltpu.roll(mid, 1, 0) + pltpu.roll(mid, width - 1, 0)) - 4.0 * mid
        return mid + cs[0, r, cols] * spread + cs[1, r, cols]

    for a in (-1, 1):
        lines = {}
        for off in range(-LATE, LATE + 1):
            r = (TOP + SKY - 1 if a < 0 else TOP + ROWS - SKY) + off
            lines[r] = dt[0, r, block]
        for level in range(LATE):
            lines = {r: later(lines[r - 1], lines[r], lines[r + 1], r, block) for r in lines if r - 1 in lines and r + 1 in lines}
            ahead[(a + 1) // 2, level] = lines[TOP + SKY - 1 if a < 0 else TOP + ROWS - SKY]

    near = (py > 0).astype(jnp.int32) + (py < npy - 1).astype(jnp.int32)
    beside = (px > 0).astype(jnp.int32) + (px < npx - 1).astype(jnp.int32)
    with jax.named_scope("barrier"):
        pl.semaphore_wait(barrier, (near + 1) * (beside + 1) - 1 + XS - 1 + len(beyond))

    def tell(n, away):
        for k in (away, zs - away):
            pl.semaphore_signal(token.at[n], inc=1, device_id=zpeer(k), device_id_type=MESH)

    if rounds:
        tell(0, 1)

    def halo(a, b, group):
        to = {"py": py + a, "px": px + b}
        at = BASE[a, b] + group
        copies = []
        for which, source, target, _ in GROUPS[a, b][group]:
            if which == COEF:
                src, dst = cs.at[(slice(None), *source)], cs.at[(slice(None), *target)]
            elif which == FIELD:
                src, dst = dt.at[(0, *source)], dt.at[(0, *target)]
            else:
                src, dst = ahead.at[(a + 1) // 2], sky.at[(1 - a) // 2]
            copies.append(pltpu.make_async_remote_copy(src, dst, hs_sem.at[at], hr_sem.at[at], device_id=to, device_id_type=MESH))
        return copies

    def all_of(a, b, group, sems):
        rows, cols = area(sum(copy[3] for copy in GROUPS[a, b][group]))
        cells = dt.at[0, rows, cols]
        pltpu.make_async_copy(cells, cells, sems.at[BASE[a, b] + group]).wait()

    order = [(0, 1), (0, -1)] + [(a, b) for a, b in SIDES if a and b]
    order = [(*side, 0) for side in order] + [(a, 0, n) for n in range(3) for a in (1, -1)]
    with jax.named_scope("sends"):
        for a, b, n in order:
            @pl.when(there(a, b))
            def _():
                for copy in halo(a, b, n):
                    copy.start()

    def arrive(a, b, n=0):
        @pl.when(there(a, b))
        def _():
            all_of(-a, -b, n, hr_sem)

    def inner(first, last, low, high):
        read, kept = pl.ds(8 * first, 8 * (last - first)), pl.ds(8 * low, 8 * (high - low))
        cut = slice(8 * (low - first), 8 * (high - first))

        def line(step, above, mid, below, r):
            side = (pltpu.roll(mid, 1, 0) + pltpu.roll(mid, mid.shape[0] - 1, 0))[cut]
            mid = mid[cut]
            dt[step + 1, r, kept] = mid + cs[0, r, kept] * ((above + below) + side - 4.0 * mid) + cs[1, r, kept]

        for step in range(STEPS):
            start, count = TOP + step + 1, ROWS - 2 * (step + 1)

            @pl.loop(0, count // 2)
            def _(i):
                r = start + 2 * i
                one, two = dt[step, r, read], dt[step, r + 1, read]
                line(step, dt[step, r - 1, kept], one, two[cut], r)
                line(step, one[cut], two, dt[step, r + 2, kept], r + 1)

    with jax.named_scope("own_cols"):
        inner(1, 5, 1, 5)
    with jax.named_scope("arrive_px"):
        arrive(0, -1)
        arrive(0, 1)
    if rounds:
        with jax.named_scope("token"):
            pl.semaphore_wait(token.at[0], 2)
        if rounds > 1:
            tell(1, 2)
    with jax.named_scope("inner"):
        inner(0, 3, 0, 2)
        inner(3, 6, 4, 6)
    far = ROWS - 2 * STEPS
    zero = jnp.zeros((COLS, LEV), jnp.float32)
    place = lax.broadcasted_iota(jnp.int32, (WIDE, LEV), 0) - LEFT

    def outer(k):
        up = dt[0, TOP - k]
        down = dt[0, TOP + ROWS - 1 + k]
        for t in range(STEPS):
            r, q = TOP - k + t + 1, TOP + ROWS - 2 + k - t
            up = later(up, dt[t, r], dt[t, r + 1], r)
            down = later(dt[t, q - 1], dt[t, q], down, q)
            if k == SKY + t + 1:
                known = (place > t) & (place < COLS - 1 - t)
                edge = jnp.zeros((LEFT, LEV), jnp.float32)
                up, down = (jnp.where(known, jnp.concatenate([edge, sky[side, t], edge], axis=0), new) for side, new in ((0, up), (1, down)))
            dt[t + 1, r] = up
            dt[t + 1, q] = down

    def come(n):
        with jax.named_scope("arrive_py"):
            for a in (-1, 1):
                if n == 0:
                    for b in (-1, 1):
                        arrive(a, b)
                arrive(a, 0, n)
        with jax.named_scope("outer"):
            for k in DIAGONALS[n]:
                outer(k)

    come(0)
    with jax.named_scope("gather"):
        guess = lax.fori_loop(0, far // 4, lambda i, v: v + sum(dt[STEPS, 2 * STEPS + 4 * i + n, block] for n in range(4)), zero) * (1.0 / far)

        def gather(lines, totals):
            for line in lines:
                moved = line - guess
                totals = (totals[0] + moved, totals[1] + moved * moved)
            return totals

        totals = lax.fori_loop(0, far // 2, lambda i, t: gather([dt[STEPS, 2 * STEPS + 2 * i + n, block] for n in range(2)], t), (zero, zero))

    come(1)
    come(2)
    with jax.named_scope("part"):
        totals = gather([dt[STEPS, r, block] for n in range(STEPS) for r in (TOP + n, TOP + ROWS - 1 - n)], totals)
        offset = totals[0] * (1.0 / ROWS)
        part[0] = guess + offset
        part[1] = totals[1] - totals[0] * offset

    def send(peer, count, mine, got, phase):
        base = 0 if phase in (0, 3) else count - 1
        return [
            pltpu.make_async_remote_copy(mine, got.at[base + k - 1], ts_sem.at[phase], tr_sem.at[phase], device_id=peer(k), device_id_type=MESH)
            for k in range(1, count)
        ]

    def start(copies):
        middle = len(copies) // 2
        for k in sorted(range(len(copies)), key=lambda k: abs(k - middle)):
            copies[k].start()

    def done(got, count, phase, sems):
        base = 0 if phase in (0, 3) else count - 1
        cells = got.at[pl.ds(base, count - 1)]
        pltpu.make_async_copy(cells, cells, sems.at[phase]).wait()

    def collect(mine, got, count, phase, each):
        done(got, count, phase, tr_sem)
        base = 0 if phase in (0, 3) else count - 1
        return merged(*([mine[s]] + [got[base + k, s] for k in range(count - 1)] for s in (0, 1)), each)

    halves = [part.at[:, pl.ds(h * HALF, HALF)] for h in (0, 1)]
    cells = float(ROWS)
    xa = send(xpeer, XS, halves[0], xin, 0)
    zb = send(zpeer, zs, halves[1], zin, 1)
    xb = send(xpeer, XS, mid_part.at[1], xin, 2)
    za = send(zpeer, zs, mid_part.at[0], zin, 3)
    start(xa)
    for n in range(1, rounds):
        with jax.named_scope("token"):
            pl.semaphore_wait(token.at[n], 2)
        if n + 1 < rounds:
            tell(n + 1, 2 ** (n + 1))
    start(zb)

    @pl.loop(0, ROWS)
    def _(i):
        e_out[i] = dt[STEPS, TOP + i, block]

    for a, b, n in order:
        @pl.when(there(a, b))
        def _():
            all_of(a, b, n, hs_sem)

    with jax.named_scope("xa"):
        mid_part[0, 0], mid_part[0, 1] = collect(halves[0], xin, XS, 0, cells)
    start(za)
    with jax.named_scope("zb"):
        mid_part[1, 0], mid_part[1, 1] = collect(halves[1], zin, zs, 1, cells)
    start(xb)
    with jax.named_scope("za"):
        mean_a, spread_a = collect(mid_part.at[0], zin, zs, 3, cells * XS)
        stats[0, :HALF] = mean_a
        stats[1, :HALF] = lax.rsqrt(spread_a * (1.0 / (ROWS * npy)) + EPS)
    with jax.named_scope("xb"):
        mean_b, spread_b = collect(mid_part.at[1], xin, XS, 2, cells * zs)
        stats[0, HALF:] = mean_b
        stats[1, HALF:] = lax.rsqrt(spread_b * (1.0 / (ROWS * npy)) + EPS)
    for got, count, phase in ((xin, XS, 0), (zin, zs, 1), (xin, XS, 2), (zin, zs, 3)):
        done(got, count, phase, ts_sem)


def finish(end, stats, a_out, e_out, held, sem):
    whole = pltpu.make_async_copy(end, e_out, sem.at[0])
    whole.start()
    mean, scale = stats[0], stats[1]
    quarter = ROWS // 4
    copies = []
    for q in range(4):
        @pl.loop(q * quarter, (q + 1) * quarter)
        def _(i):
            held[i] = (end[i] - mean) * scale

        rows = pl.ds(q * quarter, quarter)
        copies.append(pltpu.make_async_copy(held.at[rows], a_out.at[rows], sem.at[1 + q]))
        copies[-1].start()
    whole.wait()
    for copy in copies:
        copy.wait()


def solution(mesh):
    npy, npx = mesh.shape["py"], mesh.shape["px"]
    zs = npy // XS

    def per_device(density, conductance, source):
        shape = jax.ShapeDtypeStruct((ROWS, COLS, LEV), jnp.float32)
        f32 = jnp.float32
        dma = pltpu.SemaphoreType.DMA
        end, stats = pl.pallas_call(
            functools.partial(kernel, npy, npx),
            name="diffuse",
            out_shape=(pltpu.VMEM((ROWS, COLS, LEV), f32), pltpu.VMEM((2, COLS, LEV), f32)),
            in_specs=[pl.BlockSpec(memory_space=pl.ANY)] * 3,
            out_specs=[pl.BlockSpec(memory_space=pltpu.VMEM)] * 2,
            scratch_shapes=[
                pltpu.VMEM((STEPS + 1, HIGH, WIDE, LEV), f32),
                pltpu.VMEM((2, HIGH, WIDE, LEV), f32),
                pltpu.VMEM((2, LATE, COLS, LEV), f32),
                pltpu.VMEM((2, LATE, COLS, LEV), f32),
                pltpu.VMEM((2, COLS, LEV), f32),
                pltpu.VMEM((2, 2, HALF, LEV), f32),
                pltpu.VMEM((2 * (XS - 1), 2, HALF, LEV), f32),
                pltpu.VMEM((2 * (zs - 1), 2, HALF, LEV), f32),
                dma((3,)), dma((COPIES,)), dma((COPIES,)),
                dma((4,)), dma((4,)), pltpu.SemaphoreType.REGULAR((2,)),
            ],
            compiler_params=pltpu.CompilerParams(collective_id=0, has_side_effects=True),
        )(density, conductance, source)
        return pl.pallas_call(
            finish,
            name="finish",
            out_shape=(shape, shape),
            in_specs=[pl.BlockSpec(memory_space=pltpu.VMEM)] * 2,
            out_specs=[pl.BlockSpec(memory_space=pl.ANY)] * 2,
            scratch_shapes=[pltpu.VMEM((ROWS, COLS, LEV), f32), dma((5,))],
        )(*(pltpu.with_memory_space_constraint(v, pltpu.VMEM) for v in (end, stats)))

    spec = P("py", "px", None)
    return jax.shard_map(per_device, mesh=mesh, in_specs=(spec,) * 3, out_specs=(spec, spec), check_vma=False)
```

```python
import functools

import jax
import jax.numpy as jnp
from jax import lax
from jax.experimental import pallas as pl
from jax.experimental.pallas import tpu as pltpu
from jax.sharding import PartitionSpec as P

STEPS = 6
EPS = 1e-4
XS = 4
ROWS, COLS, LEV = 32, 32, 128
TOP, LEFT = STEPS, 8
HIGH, WIDE = ROWS + 2 * STEPS, COLS + 2 * LEFT
HALF = COLS // 2
ROWS_OWN, ROWS_SIDE = 6, 6
NEAR_FAR = ((0, 1), (2,))
MESH = pl.DeviceIdType.MESH
SIDES = [(a, b) for a in (-1, 0, 1) for b in (-1, 0, 1) if a or b]
SKY, LATE = 4, 2
FIELD, COEF, AHEAD = 0, 1, 2
DIAGONALS = ((1, 2, 3), (4,), (5, 6))


def reach(side, size, start, first, last):
    length = last - first + 1
    if side > 0:
        return pl.ds(start + size - last, length), pl.ds(start - last, length)
    return pl.ds(start + first - 1, length), pl.ds(start + size + first - 1, length)


def halo_groups(a, b):
    def to(which, rows, cols):
        (fr, tr), (fc, tc) = rows, cols
        return which, (fr, fc), (tr, tc), fr.size * fc.size * (2 if which == COEF else 1)

    def rows_of(first, last):
        return reach(a, ROWS, TOP, first, last)

    def cols_of(first, last):
        return reach(b, COLS, LEFT, first, last)

    def same(start, size):
        return pl.ds(start, size), pl.ds(start, size)

    whole = same(LEFT, COLS)
    if a and b:
        return [[
            to(FIELD, rows_of(1, 2), cols_of(1, 5)), to(FIELD, rows_of(3, 5), cols_of(1, 3)),
            to(COEF, rows_of(1, 2), cols_of(1, 4)), to(COEF, rows_of(3, 4), cols_of(1, 2)),
        ]]
    if b:
        return [[to(FIELD, same(TOP, ROWS), cols_of(1, STEPS)), to(COEF, same(TOP, ROWS), cols_of(1, STEPS - 1))]]
    edges = []
    for left in (True, False):
        edges.append(to(FIELD, rows_of(5, 6), same(LEFT if left else LEFT + COLS - 3, 3)))
        edges.append(to(COEF, rows_of(4, 5), same(LEFT if left else LEFT + COLS - 2, 2)))
    side = same(0, LATE)
    return [
        [to(FIELD, rows_of(1, 3), whole), to(COEF, rows_of(1, 2), whole)],
        [to(FIELD, rows_of(4, 4), whole), to(COEF, rows_of(3, 3), whole)],
        edges + [to(AHEAD, side, same(0, COLS))],
    ]


NEXT = [(a, b) for a, b in SIDES if not (a and b)]
CORNERS = [(a, b) for a, b in SIDES if a and b]
GROUPS = {side: halo_groups(*side) for side in SIDES}
BASE = {}
for _side in SIDES:
    BASE[_side] = sum(len(GROUPS[s]) for s in BASE)
COPIES = sum(len(g) for g in GROUPS.values())


def area(cells):
    for rows in range(1, HIGH + 1):
        if cells % rows == 0 and cells // rows <= WIDE:
            return pl.ds(0, rows), pl.ds(0, cells // rows)
    raise ValueError(cells)


def merged(means, spreads, each):
    mean = sum(means[1:], means[0]) * (1.0 / len(means))
    spread = sum(spreads[1:], spreads[0])
    for m in means:
        spread = spread + each * (m - mean) * (m - mean)
    return mean, spread


def kernel(npy, npx, d_hbm, c_hbm, s_hbm, e_out, stats, dt, cs, sky, ahead, part, mid_part, xin, zin,
           load_sem, hs_sem, hr_sem, ts_sem, tr_sem, token, met):
    py, px = lax.axis_index("py"), lax.axis_index("px")
    zs = npy // XS
    z, x = py // XS, lax.rem(py, XS)
    rounds = 0
    while 2 ** rounds < zs // 2:
        rounds += 1
    def there(a, b):
        ok = None
        for side, at, count in ((a, py, npy), (b, px, npx)):
            if side:
                good = (at < count - 1) if side > 0 else (at > 0)
                ok = good if ok is None else ok & good
        return ok

    def xpeer(k):
        return {"py": z * XS + lax.rem(x + k, XS), "px": px}

    def zpeer(k):
        return {"py": lax.rem(z + k, zs) * XS + x, "px": px}

    def loads(first, count, sem):
        rows, cols = pl.ds(TOP + first, count), pl.ds(LEFT, COLS)
        return [
            pltpu.make_async_copy(hbm.at[pl.ds(first, count)], to.at[field, rows, cols], load_sem.at[sem])
            for hbm, to, field in ((d_hbm, dt, 0), (c_hbm, cs, 0), (s_hbm, cs, 1))
        ]

    def loaded(count, sem):
        cells = dt.at[pl.ds(0, 3), pl.ds(0, count), pl.ds(LEFT, COLS)]
        pltpu.make_async_copy(cells, cells, load_sem.at[sem]).wait()

    for load in loads(0, STEPS, 0) + loads(ROWS - STEPS, STEPS, 0):
        load.start()
    barrier = pltpu.get_barrier_semaphore()
    for a, b in NEXT:
        @pl.when(there(a, b))
        def _():
            pl.semaphore_signal(barrier, inc=1, device_id={"py": py + a, "px": px + b}, device_id_type=MESH)
    for k in range(1, XS):
        pl.semaphore_signal(barrier, inc=1, device_id=xpeer(k), device_id_type=MESH)
    beyond = sorted({1, zs - 1})
    for k in beyond:
        pl.semaphore_signal(barrier, inc=1, device_id=zpeer(k), device_id_type=MESH)

    for load in loads(STEPS, ROWS - 2 * STEPS, 1):
        load.start()

    for a in (-1, 1):
        @pl.when(jnp.logical_not(there(a, 0)))
        def _():
            rows = pl.ds(0, TOP) if a < 0 else pl.ds(TOP + ROWS, STEPS)
            dt[0, rows] = jnp.zeros((STEPS, WIDE, LEV), jnp.float32)
            cs[:, rows] = jnp.zeros((2, STEPS, WIDE, LEV), jnp.float32)
            sky[(a + 1) // 2] = jnp.zeros((LATE, COLS, LEV), jnp.float32)
    for b in (-1, 1):
        @pl.when(jnp.logical_not(there(0, b)))
        def _():
            cols = pl.ds(0, LEFT) if b < 0 else pl.ds(LEFT + COLS, LEFT)
            dt[0, :, cols] = jnp.zeros((HIGH, LEFT, LEV), jnp.float32)
            cs[:, :, cols] = jnp.zeros((2, HIGH, LEFT, LEV), jnp.float32)

    with jax.named_scope("loads"):
        loaded(2 * STEPS, 0)
    block = pl.ds(LEFT, COLS)

    def later(above, mid, below, r, cols=slice(None)):
        width = mid.shape[0]
        spread = (above + below) + (pltpu.roll(mid, 1, 0) + pltpu.roll(mid, width - 1, 0)) - 4.0 * mid
        return mid + cs[0, r, cols] * spread + cs[1, r, cols]

    for a in (-1, 1):
        lines = {}
        for off in range(-LATE, LATE + 1):
            r = (TOP + SKY - 1 if a < 0 else TOP + ROWS - SKY) + off
            lines[r] = dt[0, r, block]
        for level in range(LATE):
            lines = {r: later(lines[r - 1], lines[r], lines[r + 1], r, block) for r in lines if r - 1 in lines and r + 1 in lines}
            ahead[(a + 1) // 2, level] = lines[TOP + SKY - 1 if a < 0 else TOP + ROWS - SKY]

    near = (py > 0).astype(jnp.int32) + (py < npy - 1).astype(jnp.int32)
    beside = (px > 0).astype(jnp.int32) + (px < npx - 1).astype(jnp.int32)
    with jax.named_scope("barrier"):
        pl.semaphore_wait(barrier, near + beside + XS - 1 + len(beyond))

    def tell(n, away):
        for k in (away, zs - away):
            pl.semaphore_signal(token.at[n], inc=1, device_id=zpeer(k), device_id_type=MESH)

    if rounds:
        tell(0, 1)
    for b in (-1, 1):
        @pl.when(there(0, b))
        def _():
            pl.semaphore_signal(met, inc=1, device_id={"py": py, "px": px + b}, device_id_type=MESH)

    def halo(a, b, group):
        to = {"py": py + a, "px": px + b}
        at = BASE[a, b] + group
        copies = []
        for which, source, target, _ in GROUPS[a, b][group]:
            if which == COEF:
                src, dst = cs.at[(slice(None), *source)], cs.at[(slice(None), *target)]
            elif which == FIELD:
                src, dst = dt.at[(0, *source)], dt.at[(0, *target)]
            else:
                src, dst = ahead.at[(a + 1) // 2], sky.at[(1 - a) // 2]
            copies.append(pltpu.make_async_remote_copy(src, dst, hs_sem.at[at], hr_sem.at[at], device_id=to, device_id_type=MESH))
        return copies

    def all_of(a, b, group, sems):
        rows, cols = area(sum(copy[3] for copy in GROUPS[a, b][group]))
        cells = dt.at[0, rows, cols]
        pltpu.make_async_copy(cells, cells, sems.at[BASE[a, b] + group]).wait()

    beside_sends = [(0, 1, 0), (0, -1, 0)]
    corner_sends = [(a, b, 0) for a, b in CORNERS]
    near_sends, far_sends = ([(a, 0, n) for n in groups for a in (1, -1)] for groups in NEAR_FAR)

    def send_halo(sends):
        for a, b, n in sends:
            @pl.when(there(a, b))
            def _():
                for copy in halo(a, b, n):
                    copy.start()

    with jax.named_scope("sends"):
        send_halo(near_sends)

    with jax.named_scope("loads2"):
        loaded(ROWS - 2 * STEPS, 1)
    send_halo(beside_sends)

    def arrive(a, b, n=0):
        @pl.when(there(a, b))
        def _():
            all_of(-a, -b, n, hr_sem)

    def inner(strips, rows):
        def lines(step, r, first, last, low, high):
            read, kept = pl.ds(8 * first, 8 * (last - first)), pl.ds(8 * low, 8 * (high - low))
            cut = slice(8 * (low - first), 8 * (high - first))
            held = [dt[step, r + n, read] for n in range(rows)]
            cuts = [dt[step, r - 1, kept]] + [h[cut] for h in held] + [dt[step, r + rows, kept]]
            for n, mid in enumerate(held):
                side = (pltpu.roll(mid, 1, 0) + pltpu.roll(mid, mid.shape[0] - 1, 0))[cut]
                spread = (cuts[n] + cuts[n + 2]) + side - 4.0 * cuts[n + 1]
                dt[step + 1, r + n, kept] = cuts[n + 1] + cs[0, r + n, kept] * spread + cs[1, r + n, kept]

        for step in range(STEPS):
            start, count = TOP + step + 1, ROWS - 2 * (step + 1)

            @pl.loop(0, pl.cdiv(count, rows))
            def _(i):
                r = start + jnp.minimum(rows * i, count - rows)
                for strip in strips:
                    lines(step, r, *strip)

    with jax.named_scope("own_cols"):
        inner(((1, 5, 1, 5),), ROWS_OWN)
    with jax.named_scope("met"):
        pl.semaphore_wait(met, beside)
    send_halo(corner_sends)

    send_halo(far_sends)
    with jax.named_scope("arrive_px"):
        arrive(0, -1)
        arrive(0, 1)
    if rounds:
        with jax.named_scope("token"):
            pl.semaphore_wait(token.at[0], 2)
        if rounds > 1:
            tell(1, 2)
    with jax.named_scope("inner"):
        inner(((0, 3, 0, 2), (3, 6, 4, 6)), ROWS_SIDE)
    far = ROWS - 2 * STEPS
    zero = jnp.zeros((COLS, LEV), jnp.float32)
    place = lax.broadcasted_iota(jnp.int32, (WIDE, LEV), 0) - LEFT

    def outer(k):
        up = dt[0, TOP - k]
        down = dt[0, TOP + ROWS - 1 + k]
        for t in range(STEPS):
            r, q = TOP - k + t + 1, TOP + ROWS - 2 + k - t
            up = later(up, dt[t, r], dt[t, r + 1], r)
            down = later(dt[t, q - 1], dt[t, q], down, q)
            if k == SKY + t + 1:
                known = (place > t) & (place < COLS - 1 - t)
                edge = jnp.zeros((LEFT, LEV), jnp.float32)
                up, down = (jnp.where(known, jnp.concatenate([edge, sky[side, t], edge], axis=0), new) for side, new in ((0, up), (1, down)))
            dt[t + 1, r] = up
            dt[t + 1, q] = down

    def come(n):
        with jax.named_scope("arrive_py"):
            for a in (-1, 1):
                if n == 0:
                    for b in (-1, 1):
                        arrive(a, b)
                arrive(a, 0, n)
        with jax.named_scope("outer"):
            for k in DIAGONALS[n]:
                outer(k)

    come(0)
    with jax.named_scope("gather"):
        guess = lax.fori_loop(0, far // 4, lambda i, v: v + sum(dt[STEPS, 2 * STEPS + 4 * i + n, block] for n in range(4)), zero) * (1.0 / far)

        def gather(lines, totals):
            for line in lines:
                moved = line - guess
                totals = (totals[0] + moved, totals[1] + moved * moved)
            return totals

        totals = lax.fori_loop(0, far // 2, lambda i, t: gather([dt[STEPS, 2 * STEPS + 2 * i + n, block] for n in range(2)], t), (zero, zero))

    come(1)
    come(2)
    with jax.named_scope("part"):
        totals = gather([dt[STEPS, r, block] for n in range(STEPS) for r in (TOP + n, TOP + ROWS - 1 - n)], totals)
        offset = totals[0] * (1.0 / ROWS)
        part[0] = guess + offset
        part[1] = totals[1] - totals[0] * offset

    def send(peer, count, mine, got, phase):
        base = 0 if phase in (0, 3) else count - 1
        return [
            pltpu.make_async_remote_copy(mine, got.at[base + k - 1], ts_sem.at[phase], tr_sem.at[phase], device_id=peer(k), device_id_type=MESH)
            for k in range(1, count)
        ]

    def start(copies):
        middle = len(copies) // 2
        for k in sorted(range(len(copies)), key=lambda k: abs(k - middle)):
            copies[k].start()

    def done(got, count, phase, sems):
        base = 0 if phase in (0, 3) else count - 1
        cells = got.at[pl.ds(base, count - 1)]
        pltpu.make_async_copy(cells, cells, sems.at[phase]).wait()

    def collect(mine, got, count, phase, each):
        done(got, count, phase, tr_sem)
        base = 0 if phase in (0, 3) else count - 1
        return merged(*([mine[s]] + [got[base + k, s] for k in range(count - 1)] for s in (0, 1)), each)

    halves = [part.at[:, pl.ds(h * HALF, HALF)] for h in (0, 1)]
    cells = float(ROWS)
    xa = send(xpeer, XS, halves[0], xin, 0)
    zb = send(zpeer, zs, halves[1], zin, 1)
    xb = send(xpeer, XS, mid_part.at[1], xin, 2)
    za = send(zpeer, zs, mid_part.at[0], zin, 3)
    start(xa)
    for n in range(1, rounds):
        with jax.named_scope("token"):
            pl.semaphore_wait(token.at[n], 2)
        if n + 1 < rounds:
            tell(n + 1, 2 ** (n + 1))
    start(zb)

    @pl.loop(0, ROWS)
    def _(i):
        e_out[i] = dt[STEPS, TOP + i, block]

    for a, b, n in beside_sends + corner_sends + near_sends + far_sends:
        @pl.when(there(a, b))
        def _():
            all_of(a, b, n, hs_sem)

    with jax.named_scope("xa"):
        mid_part[0, 0], mid_part[0, 1] = collect(halves[0], xin, XS, 0, cells)
    start(za)
    with jax.named_scope("zb"):
        mid_part[1, 0], mid_part[1, 1] = collect(halves[1], zin, zs, 1, cells)
    start(xb)
    with jax.named_scope("za"):
        mean_a, spread_a = collect(mid_part.at[0], zin, zs, 3, cells * XS)
        stats[0, :HALF] = mean_a
        stats[1, :HALF] = lax.rsqrt(spread_a * (1.0 / (ROWS * npy)) + EPS)
    with jax.named_scope("xb"):
        mean_b, spread_b = collect(mid_part.at[1], xin, XS, 2, cells * zs)
        stats[0, HALF:] = mean_b
        stats[1, HALF:] = lax.rsqrt(spread_b * (1.0 / (ROWS * npy)) + EPS)
    for got, count, phase in ((xin, XS, 0), (zin, zs, 1), (xin, XS, 2), (zin, zs, 3)):
        done(got, count, phase, ts_sem)


def finish(end, stats, a_out, e_out, held, sem):
    whole = pltpu.make_async_copy(end, e_out, sem.at[0])
    whole.start()
    mean, scale = stats[0], stats[1]
    quarter = ROWS // 4
    copies = []
    for q in range(4):
        @pl.loop(q * quarter, (q + 1) * quarter)
        def _(i):
            held[i] = (end[i] - mean) * scale

        rows = pl.ds(q * quarter, quarter)
        copies.append(pltpu.make_async_copy(held.at[rows], a_out.at[rows], sem.at[1 + q]))
        copies[-1].start()
    whole.wait()
    for copy in copies:
        copy.wait()


def solution(mesh):
    npy, npx = mesh.shape["py"], mesh.shape["px"]
    zs = npy // XS

    def per_device(density, conductance, source):
        shape = jax.ShapeDtypeStruct((ROWS, COLS, LEV), jnp.float32)
        f32 = jnp.float32
        dma = pltpu.SemaphoreType.DMA
        end, stats = pl.pallas_call(
            functools.partial(kernel, npy, npx),
            name="diffuse",
            out_shape=(pltpu.VMEM((ROWS, COLS, LEV), f32), pltpu.VMEM((2, COLS, LEV), f32)),
            in_specs=[pl.BlockSpec(memory_space=pl.ANY)] * 3,
            out_specs=[pl.BlockSpec(memory_space=pltpu.VMEM)] * 2,
            scratch_shapes=[
                pltpu.VMEM((STEPS + 1, HIGH, WIDE, LEV), f32),
                pltpu.VMEM((2, HIGH, WIDE, LEV), f32),
                pltpu.VMEM((2, LATE, COLS, LEV), f32),
                pltpu.VMEM((2, LATE, COLS, LEV), f32),
                pltpu.VMEM((2, COLS, LEV), f32),
                pltpu.VMEM((2, 2, HALF, LEV), f32),
                pltpu.VMEM((2 * (XS - 1), 2, HALF, LEV), f32),
                pltpu.VMEM((2 * (zs - 1), 2, HALF, LEV), f32),
                dma((2,)), dma((COPIES,)), dma((COPIES,)),
                dma((4,)), dma((4,)), pltpu.SemaphoreType.REGULAR((2,)), pltpu.SemaphoreType.REGULAR,
            ],
            compiler_params=pltpu.CompilerParams(collective_id=0, has_side_effects=True),
        )(density, conductance, source)
        return pl.pallas_call(
            finish,
            name="finish",
            out_shape=(shape, shape),
            in_specs=[pl.BlockSpec(memory_space=pltpu.VMEM)] * 2,
            out_specs=[pl.BlockSpec(memory_space=pl.ANY)] * 2,
            scratch_shapes=[pltpu.VMEM((ROWS, COLS, LEV), f32), dma((5,))],
        )(*(pltpu.with_memory_space_constraint(v, pltpu.VMEM) for v in (end, stats)))

    spec = P("py", "px", None)
    return jax.shard_map(per_device, mesh=mesh, in_specs=(spec,) * 3, out_specs=(spec, spec), check_vma=False)
```

```python
import functools

import jax
import jax.numpy as jnp
from jax import lax
from jax.experimental import pallas as pl
from jax.experimental.pallas import tpu as pltpu
from jax.sharding import PartitionSpec as P

STEPS = 6
EPS = 1e-4
XS = 4
ROWS, COLS, LEV = 32, 32, 128
TOP, LEFT = STEPS, 8
HIGH, WIDE = ROWS + 2 * STEPS, COLS + 2 * LEFT
HALF = COLS // 2
ROWS_OWN, ROWS_SIDE = 6, 6
X_ORDER = (0, 1, 3, 2)
NEAR_FAR = ((0, 1), (2,))
MESH = pl.DeviceIdType.MESH
SIDES = [(a, b) for a in (-1, 0, 1) for b in (-1, 0, 1) if a or b]
SKY, LATE = 4, 2
FIELD, COEF, AHEAD = 0, 1, 2
DIAGONALS = ((1, 2, 3), (4,), (5, 6))


def reach(side, size, start, first, last):
    length = last - first + 1
    if side > 0:
        return pl.ds(start + size - last, length), pl.ds(start - last, length)
    return pl.ds(start + first - 1, length), pl.ds(start + size + first - 1, length)


def halo_groups(a, b):
    def to(which, rows, cols):
        (fr, tr), (fc, tc) = rows, cols
        return which, (fr, fc), (tr, tc), fr.size * fc.size * (2 if which == COEF else 1)

    def rows_of(first, last):
        return reach(a, ROWS, TOP, first, last)

    def cols_of(first, last):
        return reach(b, COLS, LEFT, first, last)

    def same(start, size):
        return pl.ds(start, size), pl.ds(start, size)

    whole = same(LEFT, COLS)
    if a and b:
        return [[
            to(FIELD, rows_of(1, 2), cols_of(1, 5)), to(FIELD, rows_of(3, 5), cols_of(1, 3)),
            to(COEF, rows_of(1, 2), cols_of(1, 4)), to(COEF, rows_of(3, 4), cols_of(1, 2)),
        ]]
    if b:
        return [[to(FIELD, same(TOP, ROWS), cols_of(1, STEPS)), to(COEF, same(TOP, ROWS), cols_of(1, STEPS - 1))]]
    edges = []
    for left in (True, False):
        edges.append(to(FIELD, rows_of(5, 6), same(LEFT if left else LEFT + COLS - 3, 3)))
        edges.append(to(COEF, rows_of(4, 5), same(LEFT if left else LEFT + COLS - 2, 2)))
    side = same(0, LATE)
    return [
        [to(FIELD, rows_of(1, 3), whole), to(COEF, rows_of(1, 2), whole)],
        [to(FIELD, rows_of(4, 4), whole), to(COEF, rows_of(3, 3), whole)],
        edges + [to(AHEAD, side, same(0, COLS))],
    ]


NEXT = [(a, b) for a, b in SIDES if not (a and b)]
CORNERS = [(a, b) for a, b in SIDES if a and b]
GROUPS = {side: halo_groups(*side) for side in SIDES}
BASE = {}
for _side in SIDES:
    BASE[_side] = sum(len(GROUPS[s]) for s in BASE)
COPIES = sum(len(g) for g in GROUPS.values())


def area(cells):
    for rows in range(1, HIGH + 1):
        if cells % rows == 0 and cells // rows <= WIDE:
            return pl.ds(0, rows), pl.ds(0, cells // rows)
    raise ValueError(cells)


def merged(means, spreads, each):
    mean = sum(means[1:], means[0]) * (1.0 / len(means))
    spread = sum(spreads[1:], spreads[0])
    for m in means:
        spread = spread + each * (m - mean) * (m - mean)
    return mean, spread


def kernel(npy, npx, d_hbm, c_hbm, s_hbm, e_out, stats, dt, cs, sky, ahead, part, mid_part, xin, zin,
           load_sem, hs_sem, hr_sem, ts_sem, tr_sem, token, met):
    py, px = lax.axis_index("py"), lax.axis_index("px")
    zs = npy // XS
    z, x = py // XS, lax.rem(py, XS)
    rounds = 0
    while 2 ** rounds < zs // 2:
        rounds += 1
    def there(a, b):
        ok = None
        for side, at, count in ((a, py, npy), (b, px, npx)):
            if side:
                good = (at < count - 1) if side > 0 else (at > 0)
                ok = good if ok is None else ok & good
        return ok

    def xpeer(k):
        return {"py": z * XS + lax.rem(x + k, XS), "px": px}

    def zpeer(k):
        return {"py": lax.rem(z + k, zs) * XS + x, "px": px}

    def loads(first, count, sem):
        rows, cols = pl.ds(TOP + first, count), pl.ds(LEFT, COLS)
        return [
            pltpu.make_async_copy(hbm.at[pl.ds(first, count)], to.at[field, rows, cols], load_sem.at[sem])
            for hbm, to, field in ((d_hbm, dt, 0), (c_hbm, cs, 0), (s_hbm, cs, 1))
        ]

    def loaded(count, sem):
        cells = dt.at[pl.ds(0, 3), pl.ds(0, count), pl.ds(LEFT, COLS)]
        pltpu.make_async_copy(cells, cells, load_sem.at[sem]).wait()

    for load in loads(0, STEPS, 0) + loads(ROWS - STEPS, STEPS, 0):
        load.start()
    barrier = pltpu.get_barrier_semaphore()
    for a, b in NEXT:
        @pl.when(there(a, b))
        def _():
            pl.semaphore_signal(barrier, inc=1, device_id={"py": py + a, "px": px + b}, device_id_type=MESH)
    for k in range(1, XS):
        pl.semaphore_signal(barrier, inc=1, device_id=xpeer(k), device_id_type=MESH)
    beyond = sorted({1, zs - 1})
    for k in beyond:
        pl.semaphore_signal(barrier, inc=1, device_id=zpeer(k), device_id_type=MESH)

    for load in loads(STEPS, ROWS - 2 * STEPS, 1):
        load.start()

    for a in (-1, 1):
        @pl.when(jnp.logical_not(there(a, 0)))
        def _():
            rows = pl.ds(0, TOP) if a < 0 else pl.ds(TOP + ROWS, STEPS)
            dt[0, rows] = jnp.zeros((STEPS, WIDE, LEV), jnp.float32)
            cs[:, rows] = jnp.zeros((2, STEPS, WIDE, LEV), jnp.float32)
            sky[(a + 1) // 2] = jnp.zeros((LATE, COLS, LEV), jnp.float32)
    for b in (-1, 1):
        @pl.when(jnp.logical_not(there(0, b)))
        def _():
            cols = pl.ds(0, LEFT) if b < 0 else pl.ds(LEFT + COLS, LEFT)
            dt[0, :, cols] = jnp.zeros((HIGH, LEFT, LEV), jnp.float32)
            cs[:, :, cols] = jnp.zeros((2, HIGH, LEFT, LEV), jnp.float32)

    with jax.named_scope("loads"):
        loaded(2 * STEPS, 0)
    block = pl.ds(LEFT, COLS)

    def later(above, mid, below, r, cols=slice(None)):
        width = mid.shape[0]
        spread = (above + below) + (pltpu.roll(mid, 1, 0) + pltpu.roll(mid, width - 1, 0)) - 4.0 * mid
        return mid + cs[0, r, cols] * spread + cs[1, r, cols]

    for a in (-1, 1):
        lines = {}
        for off in range(-LATE, LATE + 1):
            r = (TOP + SKY - 1 if a < 0 else TOP + ROWS - SKY) + off
            lines[r] = dt[0, r, block]
        for level in range(LATE):
            lines = {r: later(lines[r - 1], lines[r], lines[r + 1], r, block) for r in lines if r - 1 in lines and r + 1 in lines}
            ahead[(a + 1) // 2, level] = lines[TOP + SKY - 1 if a < 0 else TOP + ROWS - SKY]

    near = (py > 0).astype(jnp.int32) + (py < npy - 1).astype(jnp.int32)
    beside = (px > 0).astype(jnp.int32) + (px < npx - 1).astype(jnp.int32)
    with jax.named_scope("barrier"):
        pl.semaphore_wait(barrier, near + beside + XS - 1 + len(beyond))

    def tell(n, away):
        for k in (away, zs - away):
            pl.semaphore_signal(token.at[n], inc=1, device_id=zpeer(k), device_id_type=MESH)

    if rounds:
        tell(0, 1)
    for b in (-1, 1):
        @pl.when(there(0, b))
        def _():
            pl.semaphore_signal(met, inc=1, device_id={"py": py, "px": px + b}, device_id_type=MESH)

    def halo(a, b, group):
        to = {"py": py + a, "px": px + b}
        at = BASE[a, b] + group
        copies = []
        for which, source, target, _ in GROUPS[a, b][group]:
            if which == COEF:
                src, dst = cs.at[(slice(None), *source)], cs.at[(slice(None), *target)]
            elif which == FIELD:
                src, dst = dt.at[(0, *source)], dt.at[(0, *target)]
            else:
                src, dst = ahead.at[(a + 1) // 2], sky.at[(1 - a) // 2]
            copies.append(pltpu.make_async_remote_copy(src, dst, hs_sem.at[at], hr_sem.at[at], device_id=to, device_id_type=MESH))
        return copies

    def all_of(a, b, group, sems):
        rows, cols = area(sum(copy[3] for copy in GROUPS[a, b][group]))
        cells = dt.at[0, rows, cols]
        pltpu.make_async_copy(cells, cells, sems.at[BASE[a, b] + group]).wait()

    beside_sends = [(0, 1, 0), (0, -1, 0)]
    corner_sends = [(a, b, 0) for a, b in CORNERS]
    near_sends, far_sends = ([(a, 0, n) for n in groups for a in (1, -1)] for groups in NEAR_FAR)

    def send_halo(sends):
        for a, b, n in sends:
            @pl.when(there(a, b))
            def _():
                for copy in halo(a, b, n):
                    copy.start()

    with jax.named_scope("sends"):
        send_halo(near_sends)

    with jax.named_scope("loads2"):
        loaded(ROWS - 2 * STEPS, 1)
    send_halo(beside_sends)

    def arrive(a, b, n=0):
        @pl.when(there(a, b))
        def _():
            all_of(-a, -b, n, hr_sem)

    def inner(strips, rows):
        def lines(step, r, first, last, low, high):
            read, kept = pl.ds(8 * first, 8 * (last - first)), pl.ds(8 * low, 8 * (high - low))
            cut = slice(8 * (low - first), 8 * (high - first))
            held = [dt[step, r + n, read] for n in range(rows)]
            cuts = [dt[step, r - 1, kept]] + [h[cut] for h in held] + [dt[step, r + rows, kept]]
            for n, mid in enumerate(held):
                side = (pltpu.roll(mid, 1, 0) + pltpu.roll(mid, mid.shape[0] - 1, 0))[cut]
                spread = (cuts[n] + cuts[n + 2]) + side - 4.0 * cuts[n + 1]
                dt[step + 1, r + n, kept] = cuts[n + 1] + cs[0, r + n, kept] * spread + cs[1, r + n, kept]

        for step in range(STEPS):
            start, count = TOP + step + 1, ROWS - 2 * (step + 1)

            @pl.loop(0, pl.cdiv(count, rows))
            def _(i):
                r = start + jnp.minimum(rows * i, count - rows)
                for strip in strips:
                    lines(step, r, *strip)

    with jax.named_scope("own_cols"):
        inner(((1, 5, 1, 5),), ROWS_OWN)
    with jax.named_scope("met"):
        pl.semaphore_wait(met, beside)
    send_halo(corner_sends)

    send_halo(far_sends)
    with jax.named_scope("arrive_px"):
        arrive(0, -1)
        arrive(0, 1)
    if rounds:
        with jax.named_scope("token"):
            pl.semaphore_wait(token.at[0], 2)
        if rounds > 1:
            tell(1, 2)
    with jax.named_scope("inner"):
        inner(((0, 3, 0, 2), (3, 6, 4, 6)), ROWS_SIDE)
    far = ROWS - 2 * STEPS
    zero = jnp.zeros((COLS, LEV), jnp.float32)
    place = lax.broadcasted_iota(jnp.int32, (WIDE, LEV), 0) - LEFT

    def outer(k):
        up = dt[0, TOP - k]
        down = dt[0, TOP + ROWS - 1 + k]
        for t in range(STEPS):
            r, q = TOP - k + t + 1, TOP + ROWS - 2 + k - t
            up = later(up, dt[t, r], dt[t, r + 1], r)
            down = later(dt[t, q - 1], dt[t, q], down, q)
            if k == SKY + t + 1:
                known = (place > t) & (place < COLS - 1 - t)
                edge = jnp.zeros((LEFT, LEV), jnp.float32)
                up, down = (jnp.where(known, jnp.concatenate([edge, sky[side, t], edge], axis=0), new) for side, new in ((0, up), (1, down)))
            dt[t + 1, r] = up
            dt[t + 1, q] = down

    def come(n):
        with jax.named_scope("arrive_py"):
            for a in (-1, 1):
                if n == 0:
                    for b in (-1, 1):
                        arrive(a, b)
                arrive(a, 0, n)
        with jax.named_scope("outer"):
            for k in DIAGONALS[n]:
                outer(k)

    come(0)
    with jax.named_scope("gather"):
        guess = lax.fori_loop(0, far // 4, lambda i, v: v + sum(dt[STEPS, 2 * STEPS + 4 * i + n, block] for n in range(4)), zero) * (1.0 / far)

        def gather(lines, totals):
            for line in lines:
                moved = line - guess
                totals = (totals[0] + moved, totals[1] + moved * moved)
            return totals

        totals = lax.fori_loop(0, far // 2, lambda i, t: gather([dt[STEPS, 2 * STEPS + 2 * i + n, block] for n in range(2)], t), (zero, zero))

    come(1)
    come(2)
    with jax.named_scope("part"):
        totals = gather([dt[STEPS, r, block] for n in range(STEPS) for r in (TOP + n, TOP + ROWS - 1 - n)], totals)
        offset = totals[0] * (1.0 / ROWS)
        part[0] = guess + offset
        part[1] = totals[1] - totals[0] * offset

    def start(mine, got, count, phase, targets):
        along_x = count == XS
        base, here = (0 if phase in (0, 3) else count - 1), (x if along_x else z)
        for target in targets:
            @pl.when(here != target)
            def _():
                at = base + lax.rem(target - here + count, count) - 1
                to = z * XS + target if along_x else target * XS + x
                pltpu.make_async_remote_copy(mine, got.at[at], ts_sem.at[phase], tr_sem.at[phase], device_id={"py": to, "px": px}, device_id_type=MESH).start()

    def done(got, count, phase, sems):
        base = 0 if phase in (0, 3) else count - 1
        cells = got.at[pl.ds(base, count - 1)]
        pltpu.make_async_copy(cells, cells, sems.at[phase]).wait()

    def collect(mine, got, count, phase, each):
        done(got, count, phase, tr_sem)
        base = 0 if phase in (0, 3) else count - 1
        return merged(*([mine[s]] + [got[base + k, s] for k in range(count - 1)] for s in (0, 1)), each)

    halves = [part.at[:, pl.ds(h * HALF, HALF)] for h in (0, 1)]
    cells = float(ROWS)
    start(halves[0], xin, XS, 0, X_ORDER)
    for n in range(1, rounds):
        with jax.named_scope("token"):
            pl.semaphore_wait(token.at[n], 2)
        if n + 1 < rounds:
            tell(n + 1, 2 ** (n + 1))
    start(halves[1], zin, zs, 1, range(zs))

    @pl.loop(0, ROWS)
    def _(i):
        e_out[i] = dt[STEPS, TOP + i, block]

    for a, b, n in beside_sends + corner_sends + near_sends + far_sends:
        @pl.when(there(a, b))
        def _():
            all_of(a, b, n, hs_sem)

    with jax.named_scope("xa"):
        mid_part[0, 0], mid_part[0, 1] = collect(halves[0], xin, XS, 0, cells)
    start(mid_part.at[0], zin, zs, 3, range(zs))
    with jax.named_scope("zb"):
        mid_part[1, 0], mid_part[1, 1] = collect(halves[1], zin, zs, 1, cells)
    start(mid_part.at[1], xin, XS, 2, X_ORDER)
    with jax.named_scope("za"):
        mean_a, spread_a = collect(mid_part.at[0], zin, zs, 3, cells * XS)
        stats[0, :HALF] = mean_a
        stats[1, :HALF] = lax.rsqrt(spread_a * (1.0 / (ROWS * npy)) + EPS)
    with jax.named_scope("xb"):
        mean_b, spread_b = collect(mid_part.at[1], xin, XS, 2, cells * zs)
        stats[0, HALF:] = mean_b
        stats[1, HALF:] = lax.rsqrt(spread_b * (1.0 / (ROWS * npy)) + EPS)
    for got, count, phase in ((xin, XS, 0), (zin, zs, 1), (xin, XS, 2), (zin, zs, 3)):
        done(got, count, phase, ts_sem)


def finish(end, stats, a_out, e_out, held, sem):
    whole = pltpu.make_async_copy(end, e_out, sem.at[0])
    whole.start()
    mean, scale = stats[0], stats[1]
    quarter = ROWS // 4
    copies = []
    for q in range(4):
        @pl.loop(q * quarter, (q + 1) * quarter)
        def _(i):
            held[i] = (end[i] - mean) * scale

        rows = pl.ds(q * quarter, quarter)
        copies.append(pltpu.make_async_copy(held.at[rows], a_out.at[rows], sem.at[1 + q]))
        copies[-1].start()
    whole.wait()
    for copy in copies:
        copy.wait()


def solution(mesh):
    npy, npx = mesh.shape["py"], mesh.shape["px"]
    zs = npy // XS

    def per_device(density, conductance, source):
        shape = jax.ShapeDtypeStruct((ROWS, COLS, LEV), jnp.float32)
        f32 = jnp.float32
        dma = pltpu.SemaphoreType.DMA
        end, stats = pl.pallas_call(
            functools.partial(kernel, npy, npx),
            name="diffuse",
            out_shape=(pltpu.VMEM((ROWS, COLS, LEV), f32), pltpu.VMEM((2, COLS, LEV), f32)),
            in_specs=[pl.BlockSpec(memory_space=pl.ANY)] * 3,
            out_specs=[pl.BlockSpec(memory_space=pltpu.VMEM)] * 2,
            scratch_shapes=[
                pltpu.VMEM((STEPS + 1, HIGH, WIDE, LEV), f32),
                pltpu.VMEM((2, HIGH, WIDE, LEV), f32),
                pltpu.VMEM((2, LATE, COLS, LEV), f32),
                pltpu.VMEM((2, LATE, COLS, LEV), f32),
                pltpu.VMEM((2, COLS, LEV), f32),
                pltpu.VMEM((2, 2, HALF, LEV), f32),
                pltpu.VMEM((2 * (XS - 1), 2, HALF, LEV), f32),
                pltpu.VMEM((2 * (zs - 1), 2, HALF, LEV), f32),
                dma((2,)), dma((COPIES,)), dma((COPIES,)),
                dma((4,)), dma((4,)), pltpu.SemaphoreType.REGULAR((2,)), pltpu.SemaphoreType.REGULAR,
            ],
            compiler_params=pltpu.CompilerParams(collective_id=0, has_side_effects=True),
        )(density, conductance, source)
        return pl.pallas_call(
            finish,
            name="finish",
            out_shape=(shape, shape),
            in_specs=[pl.BlockSpec(memory_space=pltpu.VMEM)] * 2,
            out_specs=[pl.BlockSpec(memory_space=pl.ANY)] * 2,
            scratch_shapes=[pltpu.VMEM((ROWS, COLS, LEV), f32), dma((5,))],
        )(*(pltpu.with_memory_space_constraint(v, pltpu.VMEM) for v in (end, stats)))

    spec = P("py", "px", None)
    return jax.shard_map(per_device, mesh=mesh, in_specs=(spec,) * 3, out_specs=(spec, spec), check_vma=False)
```

```python
import functools

import jax
import jax.numpy as jnp
from jax import lax
from jax.experimental import pallas as pl
from jax.experimental.pallas import tpu as pltpu
from jax.sharding import PartitionSpec as P

STEPS = 6
EPS = 1e-4
XS = 4
ROWS, COLS, LEV = 32, 32, 128
TOP, LEFT = STEPS, 8
HIGH, WIDE = ROWS + 2 * STEPS, COLS + 2 * LEFT
HALF = COLS // 2
ROWS_OWN, ROWS_SIDE = 6, 6
X_ORDER = (0, 1, 3, 2)
NEAR_FAR = ((0, 1), (2,))
MESH = pl.DeviceIdType.MESH
SIDES = [(a, b) for a in (-1, 0, 1) for b in (-1, 0, 1) if a or b]
SKY, LATE = 4, 2
FIELD, COEF, AHEAD = 0, 1, 2
DIAGONALS = ((1, 2, 3), (4,), (5, 6))


def reach(side, size, start, first, last):
    length = last - first + 1
    if side > 0:
        return pl.ds(start + size - last, length), pl.ds(start - last, length)
    return pl.ds(start + first - 1, length), pl.ds(start + size + first - 1, length)


def halo_groups(a, b):
    def to(which, rows, cols):
        (fr, tr), (fc, tc) = rows, cols
        return which, (fr, fc), (tr, tc), fr.size * fc.size * (2 if which == COEF else 1)

    def rows_of(first, last):
        return reach(a, ROWS, TOP, first, last)

    def cols_of(first, last):
        return reach(b, COLS, LEFT, first, last)

    def same(start, size):
        return pl.ds(start, size), pl.ds(start, size)

    whole = same(LEFT, COLS)
    if a and b:
        return [[
            to(FIELD, rows_of(1, 2), cols_of(1, 5)), to(FIELD, rows_of(3, 5), cols_of(1, 3)),
            to(COEF, rows_of(1, 2), cols_of(1, 4)), to(COEF, rows_of(3, 4), cols_of(1, 2)),
        ]]
    if b:
        return [[to(FIELD, same(TOP, ROWS), cols_of(1, STEPS)), to(COEF, same(TOP, ROWS), cols_of(1, STEPS - 1))]]
    edges = []
    for left in (True, False):
        edges.append(to(FIELD, rows_of(5, 6), same(LEFT if left else LEFT + COLS - 3, 3)))
        edges.append(to(COEF, rows_of(4, 5), same(LEFT if left else LEFT + COLS - 2, 2)))
    side = same(0, LATE)
    return [
        [to(FIELD, rows_of(1, 3), whole), to(COEF, rows_of(1, 2), whole)],
        [to(FIELD, rows_of(4, 4), whole), to(COEF, rows_of(3, 3), whole)],
        edges + [to(AHEAD, side, same(0, COLS))],
    ]


NEXT = [(a, b) for a, b in SIDES if not (a and b)]
CORNERS = [(a, b) for a, b in SIDES if a and b]
GROUPS = {side: halo_groups(*side) for side in SIDES}
BASE = {}
for _side in SIDES:
    BASE[_side] = sum(len(GROUPS[s]) for s in BASE)
COPIES = sum(len(g) for g in GROUPS.values())


def area(cells):
    for rows in range(1, HIGH + 1):
        if cells % rows == 0 and cells // rows <= WIDE:
            return pl.ds(0, rows), pl.ds(0, cells // rows)
    raise ValueError(cells)


def merged(means, spreads, each):
    mean = sum(means[1:], means[0]) * (1.0 / len(means))
    spread = sum(spreads[1:], spreads[0])
    for m in means:
        spread = spread + each * (m - mean) * (m - mean)
    return mean, spread


def kernel(npy, npx, d_hbm, c_hbm, s_hbm, e_out, stats, dt, cs, sky, ahead, part, mid_part, xin, zin,
           load_sem, hs_sem, hr_sem, ts_sem, tr_sem, token, met):
    py, px = lax.axis_index("py"), lax.axis_index("px")
    zs = npy // XS
    z, x = py // XS, lax.rem(py, XS)
    rounds = 0
    while 2 ** rounds < zs // 2:
        rounds += 1
    def there(a, b):
        ok = None
        for side, at, count in ((a, py, npy), (b, px, npx)):
            if side:
                good = (at < count - 1) if side > 0 else (at > 0)
                ok = good if ok is None else ok & good
        return ok

    def xpeer(k):
        return {"py": z * XS + lax.rem(x + k, XS), "px": px}

    def zpeer(k):
        return {"py": lax.rem(z + k, zs) * XS + x, "px": px}

    def loads(first, count, sem):
        rows, cols = pl.ds(TOP + first, count), pl.ds(LEFT, COLS)
        return [
            pltpu.make_async_copy(hbm.at[pl.ds(first, count)], to.at[field, rows, cols], load_sem.at[sem])
            for hbm, to, field in ((d_hbm, dt, 0), (c_hbm, cs, 0), (s_hbm, cs, 1))
        ]

    def loaded(count, sem):
        cells = dt.at[pl.ds(0, 3), pl.ds(0, count), pl.ds(LEFT, COLS)]
        pltpu.make_async_copy(cells, cells, load_sem.at[sem]).wait()

    for load in loads(0, STEPS, 0) + loads(ROWS - STEPS, STEPS, 0):
        load.start()
    barrier = pltpu.get_barrier_semaphore()
    for a, b in NEXT:
        @pl.when(there(a, b))
        def _():
            pl.semaphore_signal(barrier, inc=1, device_id={"py": py + a, "px": px + b}, device_id_type=MESH)
    for k in range(1, XS):
        pl.semaphore_signal(barrier, inc=1, device_id=xpeer(k), device_id_type=MESH)
    beyond = sorted({1, zs - 1})
    for k in beyond:
        pl.semaphore_signal(barrier, inc=1, device_id=zpeer(k), device_id_type=MESH)

    for load in loads(STEPS, ROWS - 2 * STEPS, 1):
        load.start()

    for a in (-1, 1):
        @pl.when(jnp.logical_not(there(a, 0)))
        def _():
            rows = pl.ds(0, TOP) if a < 0 else pl.ds(TOP + ROWS, STEPS)
            dt[0, rows] = jnp.zeros((STEPS, WIDE, LEV), jnp.float32)
            cs[:, rows] = jnp.zeros((2, STEPS, WIDE, LEV), jnp.float32)
            sky[(a + 1) // 2] = jnp.zeros((LATE, COLS, LEV), jnp.float32)
    for b in (-1, 1):
        @pl.when(jnp.logical_not(there(0, b)))
        def _():
            cols = pl.ds(0, LEFT) if b < 0 else pl.ds(LEFT + COLS, LEFT)
            dt[0, :, cols] = jnp.zeros((HIGH, LEFT, LEV), jnp.float32)
            cs[:, :, cols] = jnp.zeros((2, HIGH, LEFT, LEV), jnp.float32)

    with jax.named_scope("loads"):
        loaded(2 * STEPS, 0)
    block = pl.ds(LEFT, COLS)

    def later(above, mid, below, r, cols=slice(None)):
        width = mid.shape[0]
        spread = (above + below) + (pltpu.roll(mid, 1, 0) + pltpu.roll(mid, width - 1, 0)) - 4.0 * mid
        return mid + cs[0, r, cols] * spread + cs[1, r, cols]

    for a in (-1, 1):
        lines = {}
        for off in range(-LATE, LATE + 1):
            r = (TOP + SKY - 1 if a < 0 else TOP + ROWS - SKY) + off
            lines[r] = dt[0, r, block]
        for level in range(LATE):
            lines = {r: later(lines[r - 1], lines[r], lines[r + 1], r, block) for r in lines if r - 1 in lines and r + 1 in lines}
            ahead[(a + 1) // 2, level] = lines[TOP + SKY - 1 if a < 0 else TOP + ROWS - SKY]

    near = (py > 0).astype(jnp.int32) + (py < npy - 1).astype(jnp.int32)
    beside = (px > 0).astype(jnp.int32) + (px < npx - 1).astype(jnp.int32)
    with jax.named_scope("barrier"):
        pl.semaphore_wait(barrier, near + beside + XS - 1 + len(beyond))

    def tell(n, away):
        for k in (away, zs - away):
            pl.semaphore_signal(token.at[n], inc=1, device_id=zpeer(k), device_id_type=MESH)

    if rounds:
        tell(0, 1)
    for b in (-1, 1):
        @pl.when(there(0, b))
        def _():
            pl.semaphore_signal(met, inc=1, device_id={"py": py, "px": px + b}, device_id_type=MESH)

    def halo(a, b, group):
        to = {"py": py + a, "px": px + b}
        at = BASE[a, b] + group
        copies = []
        for which, source, target, _ in GROUPS[a, b][group]:
            if which == COEF:
                src, dst = cs.at[(slice(None), *source)], cs.at[(slice(None), *target)]
            elif which == FIELD:
                src, dst = dt.at[(0, *source)], dt.at[(0, *target)]
            else:
                src, dst = ahead.at[(a + 1) // 2], sky.at[(1 - a) // 2]
            copies.append(pltpu.make_async_remote_copy(src, dst, hs_sem.at[at], hr_sem.at[at], device_id=to, device_id_type=MESH))
        return copies

    def all_of(a, b, group, sems):
        rows, cols = area(sum(copy[3] for copy in GROUPS[a, b][group]))
        cells = dt.at[0, rows, cols]
        pltpu.make_async_copy(cells, cells, sems.at[BASE[a, b] + group]).wait()

    beside_sends = [(0, 1, 0), (0, -1, 0)]
    corner_sends = [(a, b, 0) for a, b in CORNERS]
    near_sends, far_sends = ([(a, 0, n) for n in groups for a in (1, -1)] for groups in NEAR_FAR)

    def send_halo(sends):
        for a, b, n in sends:
            @pl.when(there(a, b))
            def _():
                for copy in halo(a, b, n):
                    copy.start()

    with jax.named_scope("sends"):
        send_halo(near_sends)

    with jax.named_scope("loads2"):
        loaded(ROWS - 2 * STEPS, 1)
    send_halo(beside_sends)

    def arrive(a, b, n=0):
        @pl.when(there(a, b))
        def _():
            all_of(-a, -b, n, hr_sem)

    def inner(strips, rows):
        def lines(step, r, first, last, low, high):
            read, kept = pl.ds(8 * first, 8 * (last - first)), pl.ds(8 * low, 8 * (high - low))
            cut = slice(8 * (low - first), 8 * (high - first))
            held = [dt[step, r + n, read] for n in range(rows)]
            cuts = [dt[step, r - 1, kept]] + [h[cut] for h in held] + [dt[step, r + rows, kept]]
            for n, mid in enumerate(held):
                side = (pltpu.roll(mid, 1, 0) + pltpu.roll(mid, mid.shape[0] - 1, 0))[cut]
                spread = (cuts[n] + cuts[n + 2]) + side - 4.0 * cuts[n + 1]
                dt[step + 1, r + n, kept] = cuts[n + 1] + cs[0, r + n, kept] * spread + cs[1, r + n, kept]

        for step in range(STEPS):
            start, count = TOP + step + 1, ROWS - 2 * (step + 1)

            @pl.loop(0, pl.cdiv(count, rows))
            def _(i):
                r = start + jnp.minimum(rows * i, count - rows)
                for strip in strips:
                    lines(step, r, *strip)

    with jax.named_scope("own_cols"):
        inner(((1, 5, 1, 5),), ROWS_OWN)
    with jax.named_scope("met"):
        pl.semaphore_wait(met, beside)
    send_halo(corner_sends)

    send_halo(far_sends)
    with jax.named_scope("arrive_px"):
        arrive(0, -1)
        arrive(0, 1)
    if rounds:
        with jax.named_scope("token"):
            pl.semaphore_wait(token.at[0], 2)
        if rounds > 1:
            tell(1, 2)
    with jax.named_scope("inner"):
        inner(((0, 3, 0, 2), (3, 6, 4, 6)), ROWS_SIDE)
    far = ROWS - 2 * STEPS
    zero = jnp.zeros((COLS, LEV), jnp.float32)
    place = lax.broadcasted_iota(jnp.int32, (WIDE, LEV), 0) - LEFT

    def outer(k):
        up = dt[0, TOP - k]
        down = dt[0, TOP + ROWS - 1 + k]
        for t in range(STEPS):
            r, q = TOP - k + t + 1, TOP + ROWS - 2 + k - t
            up = later(up, dt[t, r], dt[t, r + 1], r)
            down = later(dt[t, q - 1], dt[t, q], down, q)
            if k == SKY + t + 1:
                known = (place > t) & (place < COLS - 1 - t)
                edge = jnp.zeros((LEFT, LEV), jnp.float32)
                up, down = (jnp.where(known, jnp.concatenate([edge, sky[side, t], edge], axis=0), new) for side, new in ((0, up), (1, down)))
            dt[t + 1, r] = up
            dt[t + 1, q] = down

    def come(n):
        with jax.named_scope("arrive_py"):
            for a in (-1, 1):
                if n == 0:
                    for b in (-1, 1):
                        arrive(a, b)
                arrive(a, 0, n)
        with jax.named_scope("outer"):
            for k in DIAGONALS[n]:
                outer(k)

    come(0)
    with jax.named_scope("gather"):
        guess = lax.fori_loop(0, far // 4, lambda i, v: v + sum(dt[STEPS, 2 * STEPS + 4 * i + n, block] for n in range(4)), zero) * (1.0 / far)

        def gather(lines, totals):
            for line in lines:
                moved = line - guess
                totals = (totals[0] + moved, totals[1] + moved * moved)
            return totals

        totals = lax.fori_loop(0, far // 2, lambda i, t: gather([dt[STEPS, 2 * STEPS + 2 * i + n, block] for n in range(2)], t), (zero, zero))

    come(1)
    come(2)
    with jax.named_scope("part"):
        totals = gather([dt[STEPS, r, block] for n in range(STEPS) for r in (TOP + n, TOP + ROWS - 1 - n)], totals)
        offset = totals[0] * (1.0 / ROWS)
        part[0] = guess + offset
        part[1] = totals[1] - totals[0] * offset

    def start(mine, got, count, phase, targets):
        along_x = phase in (0, 2)
        base, here = (0 if phase in (0, 3) else count - 1), (x if along_x else z)
        for target in targets:
            @pl.when(here != target)
            def _():
                at = base + lax.rem(target - here + count, count) - 1
                to = z * XS + target if along_x else target * XS + x
                pltpu.make_async_remote_copy(mine, got.at[at], ts_sem.at[phase], tr_sem.at[phase], device_id={"py": to, "px": px}, device_id_type=MESH).start()

    def done(got, count, phase, sems):
        base = 0 if phase in (0, 3) else count - 1
        cells = got.at[pl.ds(base, count - 1)]
        pltpu.make_async_copy(cells, cells, sems.at[phase]).wait()

    def collect(mine, got, count, phase, each):
        done(got, count, phase, tr_sem)
        base = 0 if phase in (0, 3) else count - 1
        return merged(*([mine[s]] + [got[base + k, s] for k in range(count - 1)] for s in (0, 1)), each)

    halves = [part.at[:, pl.ds(h * HALF, HALF)] for h in (0, 1)]
    cells = float(ROWS)
    start(halves[0], xin, XS, 0, X_ORDER)
    for n in range(1, rounds):
        with jax.named_scope("token"):
            pl.semaphore_wait(token.at[n], 2)
        if n + 1 < rounds:
            tell(n + 1, 2 ** (n + 1))
    start(halves[1], zin, zs, 1, range(zs))

    @pl.loop(0, ROWS)
    def _(i):
        e_out[i] = dt[STEPS, TOP + i, block]

    for a, b, n in beside_sends + corner_sends + near_sends + far_sends:
        @pl.when(there(a, b))
        def _():
            all_of(a, b, n, hs_sem)

    with jax.named_scope("xa"):
        mid_part[0, 0], mid_part[0, 1] = collect(halves[0], xin, XS, 0, cells)
    start(mid_part.at[0], zin, zs, 3, range(zs))
    with jax.named_scope("zb"):
        mid_part[1, 0], mid_part[1, 1] = collect(halves[1], zin, zs, 1, cells)
    start(mid_part.at[1], xin, XS, 2, X_ORDER)
    with jax.named_scope("za"):
        mean_a, spread_a = collect(mid_part.at[0], zin, zs, 3, cells * XS)
        stats[0, :HALF] = mean_a
        stats[1, :HALF] = lax.rsqrt(spread_a * (1.0 / (ROWS * npy)) + EPS)
    with jax.named_scope("xb"):
        mean_b, spread_b = collect(mid_part.at[1], xin, XS, 2, cells * zs)
        stats[0, HALF:] = mean_b
        stats[1, HALF:] = lax.rsqrt(spread_b * (1.0 / (ROWS * npy)) + EPS)
    for got, count, phase in ((xin, XS, 0), (zin, zs, 1), (xin, XS, 2), (zin, zs, 3)):
        done(got, count, phase, ts_sem)


def finish(end, stats, a_out, e_out, held, sem):
    whole = pltpu.make_async_copy(end, e_out, sem.at[0])
    whole.start()
    mean, scale = stats[0], stats[1]
    quarter = ROWS // 4
    copies = []
    for q in range(4):
        @pl.loop(q * quarter, (q + 1) * quarter)
        def _(i):
            held[i] = (end[i] - mean) * scale

        rows = pl.ds(q * quarter, quarter)
        copies.append(pltpu.make_async_copy(held.at[rows], a_out.at[rows], sem.at[1 + q]))
        copies[-1].start()
    whole.wait()
    for copy in copies:
        copy.wait()


def solution(mesh):
    npy, npx = mesh.shape["py"], mesh.shape["px"]
    zs = npy // XS

    def per_device(density, conductance, source):
        shape = jax.ShapeDtypeStruct((ROWS, COLS, LEV), jnp.float32)
        f32 = jnp.float32
        dma = pltpu.SemaphoreType.DMA
        end, stats = pl.pallas_call(
            functools.partial(kernel, npy, npx),
            name="diffuse",
            out_shape=(pltpu.VMEM((ROWS, COLS, LEV), f32), pltpu.VMEM((2, COLS, LEV), f32)),
            in_specs=[pl.BlockSpec(memory_space=pl.ANY)] * 3,
            out_specs=[pl.BlockSpec(memory_space=pltpu.VMEM)] * 2,
            scratch_shapes=[
                pltpu.VMEM((STEPS + 1, HIGH, WIDE, LEV), f32),
                pltpu.VMEM((2, HIGH, WIDE, LEV), f32),
                pltpu.VMEM((2, LATE, COLS, LEV), f32),
                pltpu.VMEM((2, LATE, COLS, LEV), f32),
                pltpu.VMEM((2, COLS, LEV), f32),
                pltpu.VMEM((2, 2, HALF, LEV), f32),
                pltpu.VMEM((2 * (XS - 1), 2, HALF, LEV), f32),
                pltpu.VMEM((2 * (zs - 1), 2, HALF, LEV), f32),
                dma((2,)), dma((COPIES,)), dma((COPIES,)),
                dma((4,)), dma((4,)), pltpu.SemaphoreType.REGULAR((2,)), pltpu.SemaphoreType.REGULAR,
            ],
            compiler_params=pltpu.CompilerParams(collective_id=0, has_side_effects=True),
        )(density, conductance, source)
        return pl.pallas_call(
            finish,
            name="finish",
            out_shape=(shape, shape),
            in_specs=[pl.BlockSpec(memory_space=pltpu.VMEM)] * 2,
            out_specs=[pl.BlockSpec(memory_space=pl.ANY)] * 2,
            scratch_shapes=[pltpu.VMEM((ROWS, COLS, LEV), f32), dma((5,))],
        )(*(pltpu.with_memory_space_constraint(v, pltpu.VMEM) for v in (end, stats)))

    spec = P("py", "px", None)
    return jax.shard_map(per_device, mesh=mesh, in_specs=(spec,) * 3, out_specs=(spec, spec), check_vma=False)
```

```python
import functools

import jax
import jax.numpy as jnp
from jax import lax
from jax.experimental import pallas as pl
from jax.experimental.pallas import tpu as pltpu
from jax.sharding import PartitionSpec as P

STEPS = 6
EPS = 1e-4
XS = 4
ROWS, COLS, LEV = 32, 32, 128
TOP, LEFT = STEPS, 8
HIGH, WIDE = ROWS + 2 * STEPS, COLS + 2 * LEFT
HALF = COLS // 2
ROWS_OWN, ROWS_SIDE = 6, 6
X_ORDER = (0, 1, 3, 2)
NEAR_FAR = ((0, 1), (2,))
MESH = pl.DeviceIdType.MESH
SIDES = [(a, b) for a in (-1, 0, 1) for b in (-1, 0, 1) if a or b]
SKY, LATE = 4, 2
FIELD, COEF, AHEAD = 0, 1, 2
DIAGONALS = ((1, 2, 3), (4,), (5, 6))


def reach(side, size, start, first, last):
    length = last - first + 1
    if side > 0:
        return pl.ds(start + size - last, length), pl.ds(start - last, length)
    return pl.ds(start + first - 1, length), pl.ds(start + size + first - 1, length)


def halo_groups(a, b):
    def to(which, rows, cols):
        (fr, tr), (fc, tc) = rows, cols
        return which, (fr, fc), (tr, tc), fr.size * fc.size * (2 if which == COEF else 1)

    def rows_of(first, last):
        return reach(a, ROWS, TOP, first, last)

    def cols_of(first, last):
        return reach(b, COLS, LEFT, first, last)

    def same(start, size):
        return pl.ds(start, size), pl.ds(start, size)

    whole = same(LEFT, COLS)
    if a and b:
        return [
            [to(FIELD, rows_of(r, r), cols_of(1, STEPS - r)) for r in range(1, STEPS)]
            + [to(COEF, rows_of(r, r), cols_of(1, STEPS - 1 - r)) for r in range(1, STEPS - 1)]
        ]
    if b:
        return [[to(FIELD, same(TOP, ROWS), cols_of(1, STEPS)), to(COEF, same(TOP, ROWS), cols_of(1, STEPS - 1))]]
    edges = []
    for left in (True, False):
        edges.append(to(FIELD, rows_of(5, 6), same(LEFT if left else LEFT + COLS - 3, 3)))
        edges.append(to(COEF, rows_of(4, 5), same(LEFT if left else LEFT + COLS - 2, 2)))
    side = same(0, LATE)
    return [
        [to(FIELD, rows_of(1, 3), whole), to(COEF, rows_of(1, 2), whole)],
        [to(FIELD, rows_of(4, 4), whole), to(COEF, rows_of(3, 3), whole)],
        edges + [to(AHEAD, side, same(0, COLS))],
    ]


NEXT = [(a, b) for a, b in SIDES if not (a and b)]
CORNERS = [(a, b) for a, b in SIDES if a and b]
GROUPS = {side: halo_groups(*side) for side in SIDES}
BASE = {}
for _side in SIDES:
    BASE[_side] = sum(len(GROUPS[s]) for s in BASE)
COPIES = sum(len(g) for g in GROUPS.values())


def area(cells):
    for rows in range(1, HIGH + 1):
        if cells % rows == 0 and cells // rows <= WIDE:
            return pl.ds(0, rows), pl.ds(0, cells // rows)
    raise ValueError(cells)


def merged(means, spreads, each):
    mean = sum(means[1:], means[0]) * (1.0 / len(means))
    spread = sum(spreads[1:], spreads[0])
    for m in means:
        spread = spread + each * (m - mean) * (m - mean)
    return mean, spread


def kernel(npy, npx, d_hbm, c_hbm, s_hbm, e_out, stats, dt, cs, sky, ahead, part, mid_part, xin, zin,
           load_sem, hs_sem, hr_sem, ts_sem, tr_sem, token, met):
    py, px = lax.axis_index("py"), lax.axis_index("px")
    zs = npy // XS
    z, x = py // XS, lax.rem(py, XS)
    rounds = 0
    while 2 ** rounds < zs // 2:
        rounds += 1
    def there(a, b):
        ok = None
        for side, at, count in ((a, py, npy), (b, px, npx)):
            if side:
                good = (at < count - 1) if side > 0 else (at > 0)
                ok = good if ok is None else ok & good
        return ok

    def xpeer(k):
        return {"py": z * XS + lax.rem(x + k, XS), "px": px}

    def zpeer(k):
        return {"py": lax.rem(z + k, zs) * XS + x, "px": px}

    def loads(first, count, sem):
        rows, cols = pl.ds(TOP + first, count), pl.ds(LEFT, COLS)
        return [
            pltpu.make_async_copy(hbm.at[pl.ds(first, count)], to.at[field, rows, cols], load_sem.at[sem])
            for hbm, to, field in ((d_hbm, dt, 0), (c_hbm, cs, 0), (s_hbm, cs, 1))
        ]

    def loaded(count, sem):
        cells = dt.at[pl.ds(0, 3), pl.ds(0, count), pl.ds(LEFT, COLS)]
        pltpu.make_async_copy(cells, cells, load_sem.at[sem]).wait()

    for load in loads(0, STEPS, 0) + loads(ROWS - STEPS, STEPS, 0):
        load.start()
    barrier = pltpu.get_barrier_semaphore()
    for a, b in NEXT:
        @pl.when(there(a, b))
        def _():
            pl.semaphore_signal(barrier, inc=1, device_id={"py": py + a, "px": px + b}, device_id_type=MESH)
    for k in range(1, XS):
        pl.semaphore_signal(barrier, inc=1, device_id=xpeer(k), device_id_type=MESH)
    beyond = sorted({1, zs - 1})
    for k in beyond:
        pl.semaphore_signal(barrier, inc=1, device_id=zpeer(k), device_id_type=MESH)

    for load in loads(STEPS, ROWS - 2 * STEPS, 1):
        load.start()

    for a in (-1, 1):
        @pl.when(jnp.logical_not(there(a, 0)))
        def _():
            rows = pl.ds(0, TOP) if a < 0 else pl.ds(TOP + ROWS, STEPS)
            dt[0, rows] = jnp.zeros((STEPS, WIDE, LEV), jnp.float32)
            cs[:, rows] = jnp.zeros((2, STEPS, WIDE, LEV), jnp.float32)
            sky[(a + 1) // 2] = jnp.zeros((LATE, COLS, LEV), jnp.float32)
    for b in (-1, 1):
        @pl.when(jnp.logical_not(there(0, b)))
        def _():
            cols = pl.ds(0, LEFT) if b < 0 else pl.ds(LEFT + COLS, LEFT)
            dt[0, :, cols] = jnp.zeros((HIGH, LEFT, LEV), jnp.float32)
            cs[:, :, cols] = jnp.zeros((2, HIGH, LEFT, LEV), jnp.float32)

    with jax.named_scope("loads"):
        loaded(2 * STEPS, 0)
    block = pl.ds(LEFT, COLS)

    def later(above, mid, below, r, cols=slice(None)):
        width = mid.shape[0]
        spread = (above + below) + (pltpu.roll(mid, 1, 0) + pltpu.roll(mid, width - 1, 0)) - 4.0 * mid
        return mid + cs[0, r, cols] * spread + cs[1, r, cols]

    for a in (-1, 1):
        lines = {}
        for off in range(-LATE, LATE + 1):
            r = (TOP + SKY - 1 if a < 0 else TOP + ROWS - SKY) + off
            lines[r] = dt[0, r, block]
        for level in range(LATE):
            lines = {r: later(lines[r - 1], lines[r], lines[r + 1], r, block) for r in lines if r - 1 in lines and r + 1 in lines}
            ahead[(a + 1) // 2, level] = lines[TOP + SKY - 1 if a < 0 else TOP + ROWS - SKY]

    near = (py > 0).astype(jnp.int32) + (py < npy - 1).astype(jnp.int32)
    beside = (px > 0).astype(jnp.int32) + (px < npx - 1).astype(jnp.int32)
    with jax.named_scope("barrier"):
        pl.semaphore_wait(barrier, near + beside + XS - 1 + len(beyond))

    def tell(n, away):
        for k in (away, zs - away):
            pl.semaphore_signal(token.at[n], inc=1, device_id=zpeer(k), device_id_type=MESH)

    if rounds:
        tell(0, 1)
    for b in (-1, 1):
        @pl.when(there(0, b))
        def _():
            pl.semaphore_signal(met, inc=1, device_id={"py": py, "px": px + b}, device_id_type=MESH)

    def halo(a, b, group):
        to = {"py": py + a, "px": px + b}
        at = BASE[a, b] + group
        copies = []
        for which, source, target, _ in GROUPS[a, b][group]:
            if which == COEF:
                src, dst = cs.at[(slice(None), *source)], cs.at[(slice(None), *target)]
            elif which == FIELD:
                src, dst = dt.at[(0, *source)], dt.at[(0, *target)]
            else:
                src, dst = ahead.at[(a + 1) // 2], sky.at[(1 - a) // 2]
            copies.append(pltpu.make_async_remote_copy(src, dst, hs_sem.at[at], hr_sem.at[at], device_id=to, device_id_type=MESH))
        return copies

    def all_of(a, b, group, sems):
        rows, cols = area(sum(copy[3] for copy in GROUPS[a, b][group]))
        cells = dt.at[0, rows, cols]
        pltpu.make_async_copy(cells, cells, sems.at[BASE[a, b] + group]).wait()

    beside_sends = [(0, 1, 0), (0, -1, 0)]
    corner_sends = [(a, b, 0) for a, b in CORNERS]
    near_sends, far_sends = ([(a, 0, n) for n in groups for a in (1, -1)] for groups in NEAR_FAR)

    def send_halo(sends):
        for a, b, n in sends:
            @pl.when(there(a, b))
            def _():
                for copy in halo(a, b, n):
                    copy.start()

    with jax.named_scope("sends"):
        send_halo(near_sends)

    with jax.named_scope("loads2"):
        loaded(ROWS - 2 * STEPS, 1)
    send_halo(beside_sends)

    def arrive(a, b, n=0):
        @pl.when(there(a, b))
        def _():
            all_of(-a, -b, n, hr_sem)

    def inner(strips, rows):
        def lines(step, r, first, last, low, high):
            read, kept = pl.ds(8 * first, 8 * (last - first)), pl.ds(8 * low, 8 * (high - low))
            cut = slice(8 * (low - first), 8 * (high - first))
            held = [dt[step, r + n, read] for n in range(rows)]
            cuts = [dt[step, r - 1, kept]] + [h[cut] for h in held] + [dt[step, r + rows, kept]]
            for n, mid in enumerate(held):
                side = (pltpu.roll(mid, 1, 0) + pltpu.roll(mid, mid.shape[0] - 1, 0))[cut]
                spread = (cuts[n] + cuts[n + 2]) + side - 4.0 * cuts[n + 1]
                dt[step + 1, r + n, kept] = cuts[n + 1] + cs[0, r + n, kept] * spread + cs[1, r + n, kept]

        for step in range(STEPS):
            start, count = TOP + step + 1, ROWS - 2 * (step + 1)

            @pl.loop(0, pl.cdiv(count, rows))
            def _(i):
                r = start + jnp.minimum(rows * i, count - rows)
                for strip in strips:
                    lines(step, r, *strip)

    with jax.named_scope("own_cols"):
        inner(((1, 5, 1, 5),), ROWS_OWN)
    with jax.named_scope("met"):
        pl.semaphore_wait(met, beside)
    send_halo(corner_sends)

    send_halo(far_sends)
    with jax.named_scope("arrive_px"):
        arrive(0, -1)
        arrive(0, 1)
    if rounds:
        with jax.named_scope("token"):
            pl.semaphore_wait(token.at[0], 2)
        if rounds > 1:
            tell(1, 2)
    with jax.named_scope("inner"):
        inner(((0, 3, 0, 2), (3, 6, 4, 6)), ROWS_SIDE)
    far = ROWS - 2 * STEPS
    zero = jnp.zeros((COLS, LEV), jnp.float32)
    place = lax.broadcasted_iota(jnp.int32, (WIDE, LEV), 0) - LEFT

    def outer(k):
        up = dt[0, TOP - k]
        down = dt[0, TOP + ROWS - 1 + k]
        for t in range(STEPS):
            r, q = TOP - k + t + 1, TOP + ROWS - 2 + k - t
            up = later(up, dt[t, r], dt[t, r + 1], r)
            down = later(dt[t, q - 1], dt[t, q], down, q)
            if k == SKY + t + 1:
                known = (place > t) & (place < COLS - 1 - t)
                edge = jnp.zeros((LEFT, LEV), jnp.float32)
                up, down = (jnp.where(known, jnp.concatenate([edge, sky[side, t], edge], axis=0), new) for side, new in ((0, up), (1, down)))
            dt[t + 1, r] = up
            dt[t + 1, q] = down

    def come(n):
        with jax.named_scope("arrive_py"):
            for a in (-1, 1):
                if n == 0:
                    for b in (-1, 1):
                        arrive(a, b)
                arrive(a, 0, n)
        with jax.named_scope("outer"):
            for k in DIAGONALS[n]:
                outer(k)

    come(0)
    with jax.named_scope("gather"):
        guess = lax.fori_loop(0, far // 4, lambda i, v: v + sum(dt[STEPS, 2 * STEPS + 4 * i + n, block] for n in range(4)), zero) * (1.0 / far)

        def gather(lines, totals):
            for line in lines:
                moved = line - guess
                totals = (totals[0] + moved, totals[1] + moved * moved)
            return totals

        totals = lax.fori_loop(0, far // 2, lambda i, t: gather([dt[STEPS, 2 * STEPS + 2 * i + n, block] for n in range(2)], t), (zero, zero))

    come(1)
    come(2)
    with jax.named_scope("part"):
        totals = gather([dt[STEPS, r, block] for n in range(STEPS) for r in (TOP + n, TOP + ROWS - 1 - n)], totals)
        offset = totals[0] * (1.0 / ROWS)
        part[0] = guess + offset
        part[1] = totals[1] - totals[0] * offset

    def start(mine, got, count, phase, targets):
        along_x = phase in (0, 2)
        base, here = (0 if phase in (0, 3) else count - 1), (x if along_x else z)
        for target in targets:
            @pl.when(here != target)
            def _():
                at = base + lax.rem(target - here + count, count) - 1
                to = z * XS + target if along_x else target * XS + x
                pltpu.make_async_remote_copy(mine, got.at[at], ts_sem.at[phase], tr_sem.at[phase], device_id={"py": to, "px": px}, device_id_type=MESH).start()

    def done(got, count, phase, sems):
        base = 0 if phase in (0, 3) else count - 1
        cells = got.at[pl.ds(base, count - 1)]
        pltpu.make_async_copy(cells, cells, sems.at[phase]).wait()

    def collect(mine, got, count, phase, each):
        done(got, count, phase, tr_sem)
        base = 0 if phase in (0, 3) else count - 1
        return merged(*([mine[s]] + [got[base + k, s] for k in range(count - 1)] for s in (0, 1)), each)

    halves = [part.at[:, pl.ds(h * HALF, HALF)] for h in (0, 1)]
    cells = float(ROWS)
    start(halves[0], xin, XS, 0, X_ORDER)
    for n in range(1, rounds):
        with jax.named_scope("token"):
            pl.semaphore_wait(token.at[n], 2)
        if n + 1 < rounds:
            tell(n + 1, 2 ** (n + 1))
    start(halves[1], zin, zs, 1, range(zs))

    @pl.loop(0, ROWS)
    def _(i):
        e_out[i] = dt[STEPS, TOP + i, block]

    for a, b, n in beside_sends + corner_sends + near_sends + far_sends:
        @pl.when(there(a, b))
        def _():
            all_of(a, b, n, hs_sem)

    with jax.named_scope("xa"):
        mid_part[0, 0], mid_part[0, 1] = collect(halves[0], xin, XS, 0, cells)
    early = z < zs // 2
    start(mid_part.at[0], zin, zs, 3, range(zs // 2))

    @pl.when(jnp.logical_not(early))
    def _():
        start(mid_part.at[0], zin, zs, 3, range(zs // 2, zs))

    with jax.named_scope("zb"):
        mid_part[1, 0], mid_part[1, 1] = collect(halves[1], zin, zs, 1, cells)
    start(mid_part.at[1], xin, XS, 2, X_ORDER)

    @pl.when(early)
    def _():
        start(mid_part.at[0], zin, zs, 3, range(zs // 2, zs))

    with jax.named_scope("za"):
        mean_a, spread_a = collect(mid_part.at[0], zin, zs, 3, cells * XS)
        stats[0, :HALF] = mean_a
        stats[1, :HALF] = lax.rsqrt(spread_a * (1.0 / (ROWS * npy)) + EPS)
    with jax.named_scope("xb"):
        mean_b, spread_b = collect(mid_part.at[1], xin, XS, 2, cells * zs)
        stats[0, HALF:] = mean_b
        stats[1, HALF:] = lax.rsqrt(spread_b * (1.0 / (ROWS * npy)) + EPS)
    for got, count, phase in ((xin, XS, 0), (zin, zs, 1), (xin, XS, 2), (zin, zs, 3)):
        done(got, count, phase, ts_sem)


def finish(end, stats, a_out, e_out, held, sem):
    whole = pltpu.make_async_copy(end, e_out, sem.at[0])
    whole.start()
    mean, scale = stats[0], stats[1]
    quarter = ROWS // 4
    copies = []
    for q in range(4):
        @pl.loop(q * quarter, (q + 1) * quarter)
        def _(i):
            held[i] = (end[i] - mean) * scale

        rows = pl.ds(q * quarter, quarter)
        copies.append(pltpu.make_async_copy(held.at[rows], a_out.at[rows], sem.at[1 + q]))
        copies[-1].start()
    whole.wait()
    for copy in copies:
        copy.wait()


def solution(mesh):
    npy, npx = mesh.shape["py"], mesh.shape["px"]
    zs = npy // XS

    def per_device(density, conductance, source):
        shape = jax.ShapeDtypeStruct((ROWS, COLS, LEV), jnp.float32)
        f32 = jnp.float32
        dma = pltpu.SemaphoreType.DMA
        end, stats = pl.pallas_call(
            functools.partial(kernel, npy, npx),
            name="diffuse",
            out_shape=(pltpu.VMEM((ROWS, COLS, LEV), f32), pltpu.VMEM((2, COLS, LEV), f32)),
            in_specs=[pl.BlockSpec(memory_space=pl.ANY)] * 3,
            out_specs=[pl.BlockSpec(memory_space=pltpu.VMEM)] * 2,
            scratch_shapes=[
                pltpu.VMEM((STEPS + 1, HIGH, WIDE, LEV), f32),
                pltpu.VMEM((2, HIGH, WIDE, LEV), f32),
                pltpu.VMEM((2, LATE, COLS, LEV), f32),
                pltpu.VMEM((2, LATE, COLS, LEV), f32),
                pltpu.VMEM((2, COLS, LEV), f32),
                pltpu.VMEM((2, 2, HALF, LEV), f32),
                pltpu.VMEM((2 * (XS - 1), 2, HALF, LEV), f32),
                pltpu.VMEM((2 * (zs - 1), 2, HALF, LEV), f32),
                dma((2,)), dma((COPIES,)), dma((COPIES,)),
                dma((4,)), dma((4,)), pltpu.SemaphoreType.REGULAR((2,)), pltpu.SemaphoreType.REGULAR,
            ],
            compiler_params=pltpu.CompilerParams(collective_id=0, has_side_effects=True),
        )(density, conductance, source)
        return pl.pallas_call(
            finish,
            name="finish",
            out_shape=(shape, shape),
            in_specs=[pl.BlockSpec(memory_space=pltpu.VMEM)] * 2,
            out_specs=[pl.BlockSpec(memory_space=pl.ANY)] * 2,
            scratch_shapes=[pltpu.VMEM((ROWS, COLS, LEV), f32), dma((5,))],
        )(*(pltpu.with_memory_space_constraint(v, pltpu.VMEM) for v in (end, stats)))

    spec = P("py", "px", None)
    return jax.shard_map(per_device, mesh=mesh, in_specs=(spec,) * 3, out_specs=(spec, spec), check_vma=False)
```

```python
import functools

import jax
import jax.numpy as jnp
from jax import lax
from jax.experimental import pallas as pl
from jax.experimental.pallas import tpu as pltpu
from jax.sharding import PartitionSpec as P

STEPS = 6
EPS = 1e-4
XS = 4
ROWS, COLS, LEV = 32, 32, 128
TOP, LEFT = STEPS, 8
HIGH, WIDE = ROWS + 2 * STEPS, COLS + 2 * LEFT
HALF = COLS // 2
ROWS_OWN, ROWS_SIDE = 10, 10
X_ORDER = (0, 3, 1, 2)
NEAR_FAR = ((0, 1), (2,))
MESH = pl.DeviceIdType.MESH
SIDES = [(a, b) for a in (-1, 0, 1) for b in (-1, 0, 1) if a or b]
SKY, LATE = 4, 2
FIELD, COEF, AHEAD = 0, 1, 2
DIAGONALS = ((1, 2, 3), (4,), (5, 6))


def reach(side, size, start, first, last):
    length = last - first + 1
    if side > 0:
        return pl.ds(start + size - last, length), pl.ds(start - last, length)
    return pl.ds(start + first - 1, length), pl.ds(start + size + first - 1, length)


def halo_groups(a, b):
    def to(which, rows, cols):
        (fr, tr), (fc, tc) = rows, cols
        return which, (fr, fc), (tr, tc), fr.size * fc.size * (2 if which == COEF else 1)

    def rows_of(first, last):
        return reach(a, ROWS, TOP, first, last)

    def cols_of(first, last):
        return reach(b, COLS, LEFT, first, last)

    def same(start, size):
        return pl.ds(start, size), pl.ds(start, size)

    whole = same(LEFT, COLS)
    if a and b:
        return [
            [to(FIELD, rows_of(r, r), cols_of(1, STEPS - r)) for r in range(1, STEPS)]
            + [to(COEF, rows_of(r, r), cols_of(1, STEPS - 1 - r)) for r in range(1, STEPS - 1)]
        ]
    if b:
        return [[to(FIELD, same(TOP, ROWS), cols_of(1, STEPS)), to(COEF, same(TOP, ROWS), cols_of(1, STEPS - 1))]]
    edges = []
    for left in (True, False):
        edges.append(to(FIELD, rows_of(5, 6), same(LEFT if left else LEFT + COLS - 3, 3)))
        edges.append(to(COEF, rows_of(4, 5), same(LEFT if left else LEFT + COLS - 2, 2)))
    side = same(0, LATE)
    return [
        [to(FIELD, rows_of(1, 3), whole), to(COEF, rows_of(1, 2), whole)],
        [to(FIELD, rows_of(4, 4), whole), to(COEF, rows_of(3, 3), whole)],
        edges + [to(AHEAD, side, same(0, COLS))],
    ]


NEXT = [(a, b) for a, b in SIDES if not (a and b)]
CORNERS = [(a, b) for a, b in SIDES if a and b]
GROUPS = {side: halo_groups(*side) for side in SIDES}
BASE = {}
for _side in SIDES:
    BASE[_side] = sum(len(GROUPS[s]) for s in BASE)
COPIES = sum(len(g) for g in GROUPS.values())


def area(cells):
    for rows in range(1, HIGH + 1):
        if cells % rows == 0 and cells // rows <= WIDE:
            return pl.ds(0, rows), pl.ds(0, cells // rows)
    raise ValueError(cells)


def merged(means, spreads, each):
    mean = sum(means[1:], means[0]) * (1.0 / len(means))
    spread = sum(spreads[1:], spreads[0])
    for m in means:
        spread = spread + each * (m - mean) * (m - mean)
    return mean, spread


def kernel(npy, npx, d_hbm, c_hbm, s_hbm, e_out, stats, dt, cs, sky, ahead, part, mid_part, xin, zin,
           load_sem, hs_sem, hr_sem, ts_sem, tr_sem, token, met):
    py, px = lax.axis_index("py"), lax.axis_index("px")
    zs = npy // XS
    z, x = py // XS, lax.rem(py, XS)
    rounds = 0
    while 2 ** rounds < zs // 2:
        rounds += 1
    def there(a, b):
        ok = None
        for side, at, count in ((a, py, npy), (b, px, npx)):
            if side:
                good = (at < count - 1) if side > 0 else (at > 0)
                ok = good if ok is None else ok & good
        return ok

    def xpeer(k):
        return {"py": z * XS + lax.rem(x + k, XS), "px": px}

    def zpeer(k):
        return {"py": lax.rem(z + k, zs) * XS + x, "px": px}

    def loads(first, count, sem):
        rows, cols = pl.ds(TOP + first, count), pl.ds(LEFT, COLS)
        return [
            pltpu.make_async_copy(hbm.at[pl.ds(first, count)], to.at[field, rows, cols], load_sem.at[sem])
            for hbm, to, field in ((d_hbm, dt, 0), (c_hbm, cs, 0), (s_hbm, cs, 1))
        ]

    def loaded(count, sem):
        cells = dt.at[pl.ds(0, 3), pl.ds(0, count), pl.ds(LEFT, COLS)]
        pltpu.make_async_copy(cells, cells, load_sem.at[sem]).wait()

    for load in loads(0, STEPS, 0) + loads(ROWS - STEPS, STEPS, 0):
        load.start()
    barrier = pltpu.get_barrier_semaphore()
    for a, b in NEXT:
        @pl.when(there(a, b))
        def _():
            pl.semaphore_signal(barrier, inc=1, device_id={"py": py + a, "px": px + b}, device_id_type=MESH)
    for k in range(1, XS):
        pl.semaphore_signal(barrier, inc=1, device_id=xpeer(k), device_id_type=MESH)
    beyond = sorted({1, zs - 1})
    for k in beyond:
        pl.semaphore_signal(barrier, inc=1, device_id=zpeer(k), device_id_type=MESH)

    for load in loads(STEPS, ROWS - 2 * STEPS, 1):
        load.start()

    for a in (-1, 1):
        @pl.when(jnp.logical_not(there(a, 0)))
        def _():
            rows = pl.ds(0, TOP) if a < 0 else pl.ds(TOP + ROWS, STEPS)
            dt[0, rows] = jnp.zeros((STEPS, WIDE, LEV), jnp.float32)
            cs[:, rows] = jnp.zeros((2, STEPS, WIDE, LEV), jnp.float32)
            sky[(a + 1) // 2] = jnp.zeros((LATE, COLS, LEV), jnp.float32)
    for b in (-1, 1):
        @pl.when(jnp.logical_not(there(0, b)))
        def _():
            cols = pl.ds(0, LEFT) if b < 0 else pl.ds(LEFT + COLS, LEFT)
            dt[0, :, cols] = jnp.zeros((HIGH, LEFT, LEV), jnp.float32)
            cs[:, :, cols] = jnp.zeros((2, HIGH, LEFT, LEV), jnp.float32)

    with jax.named_scope("loads"):
        loaded(2 * STEPS, 0)
    block = pl.ds(LEFT, COLS)

    def later(above, mid, below, r, cols=slice(None)):
        width = mid.shape[0]
        spread = (above + below) + (pltpu.roll(mid, 1, 0) + pltpu.roll(mid, width - 1, 0)) - 4.0 * mid
        return mid + cs[0, r, cols] * spread + cs[1, r, cols]

    for a in (-1, 1):
        lines = {}
        for off in range(-LATE, LATE + 1):
            r = (TOP + SKY - 1 if a < 0 else TOP + ROWS - SKY) + off
            lines[r] = dt[0, r, block]
        for level in range(LATE):
            lines = {r: later(lines[r - 1], lines[r], lines[r + 1], r, block) for r in lines if r - 1 in lines and r + 1 in lines}
            ahead[(a + 1) // 2, level] = lines[TOP + SKY - 1 if a < 0 else TOP + ROWS - SKY]

    near = (py > 0).astype(jnp.int32) + (py < npy - 1).astype(jnp.int32)
    beside = (px > 0).astype(jnp.int32) + (px < npx - 1).astype(jnp.int32)
    with jax.named_scope("barrier"):
        pl.semaphore_wait(barrier, near + beside + XS - 1 + len(beyond))

    def tell(n, away):
        for k in (away, zs - away):
            pl.semaphore_signal(token.at[n], inc=1, device_id=zpeer(k), device_id_type=MESH)

    if rounds:
        tell(0, 1)
    for b in (-1, 1):
        @pl.when(there(0, b))
        def _():
            pl.semaphore_signal(met, inc=1, device_id={"py": py, "px": px + b}, device_id_type=MESH)

    def halo(a, b, group):
        to = {"py": py + a, "px": px + b}
        at = BASE[a, b] + group
        copies = []
        for which, source, target, _ in GROUPS[a, b][group]:
            if which == COEF:
                src, dst = cs.at[(slice(None), *source)], cs.at[(slice(None), *target)]
            elif which == FIELD:
                src, dst = dt.at[(0, *source)], dt.at[(0, *target)]
            else:
                src, dst = ahead.at[(a + 1) // 2], sky.at[(1 - a) // 2]
            copies.append(pltpu.make_async_remote_copy(src, dst, hs_sem.at[at], hr_sem.at[at], device_id=to, device_id_type=MESH))
        return copies

    def all_of(a, b, group, sems):
        rows, cols = area(sum(copy[3] for copy in GROUPS[a, b][group]))
        cells = dt.at[0, rows, cols]
        pltpu.make_async_copy(cells, cells, sems.at[BASE[a, b] + group]).wait()

    beside_sends = [(0, 1, 0), (0, -1, 0)]
    corner_sends = [(a, b, 0) for a, b in CORNERS]
    near_sends, far_sends = ([(a, 0, n) for n in groups for a in (1, -1)] for groups in NEAR_FAR)

    def send_halo(sends):
        for a, b, n in sends:
            @pl.when(there(a, b))
            def _():
                for copy in halo(a, b, n):
                    copy.start()

    with jax.named_scope("sends"):
        send_halo(near_sends)

    with jax.named_scope("loads2"):
        loaded(ROWS - 2 * STEPS, 1)
    send_halo(beside_sends)

    def arrive(a, b, n=0):
        @pl.when(there(a, b))
        def _():
            all_of(-a, -b, n, hr_sem)

    def inner(strips, rows):
        def lines(step, r, first, last, low, high):
            read, kept = pl.ds(8 * first, 8 * (last - first)), pl.ds(8 * low, 8 * (high - low))
            cut = slice(8 * (low - first), 8 * (high - first))
            held = [dt[step, r + n, read] for n in range(rows)]
            cuts = [dt[step, r - 1, kept]] + [h[cut] for h in held] + [dt[step, r + rows, kept]]
            for n, mid in enumerate(held):
                side = (pltpu.roll(mid, 1, 0) + pltpu.roll(mid, mid.shape[0] - 1, 0))[cut]
                spread = (cuts[n] + cuts[n + 2]) + side - 4.0 * cuts[n + 1]
                dt[step + 1, r + n, kept] = cuts[n + 1] + cs[0, r + n, kept] * spread + cs[1, r + n, kept]

        for step in range(STEPS):
            start, count = TOP + step + 1, ROWS - 2 * (step + 1)

            @pl.loop(0, pl.cdiv(count, rows))
            def _(i):
                r = start + jnp.minimum(rows * i, count - rows)
                for strip in strips:
                    lines(step, r, *strip)

    with jax.named_scope("own_cols"):
        inner(((1, 5, 1, 5),), ROWS_OWN)
    with jax.named_scope("met"):
        pl.semaphore_wait(met, beside)
    send_halo(corner_sends)

    send_halo(far_sends)
    with jax.named_scope("arrive_px"):
        arrive(0, -1)
        arrive(0, 1)
    if rounds:
        with jax.named_scope("token"):
            pl.semaphore_wait(token.at[0], 2)
        if rounds > 1:
            tell(1, 2)
    with jax.named_scope("inner"):
        inner(((0, 3, 0, 2), (3, 6, 4, 6)), ROWS_SIDE)
    far = ROWS - 2 * STEPS
    zero = jnp.zeros((COLS, LEV), jnp.float32)
    place = lax.broadcasted_iota(jnp.int32, (WIDE, LEV), 0) - LEFT

    def outer(k):
        up = dt[0, TOP - k]
        down = dt[0, TOP + ROWS - 1 + k]
        for t in range(STEPS):
            r, q = TOP - k + t + 1, TOP + ROWS - 2 + k - t
            up = later(up, dt[t, r], dt[t, r + 1], r)
            down = later(dt[t, q - 1], dt[t, q], down, q)
            if k == SKY + t + 1:
                known = (place > t) & (place < COLS - 1 - t)
                edge = jnp.zeros((LEFT, LEV), jnp.float32)
                up, down = (jnp.where(known, jnp.concatenate([edge, sky[side, t], edge], axis=0), new) for side, new in ((0, up), (1, down)))
            dt[t + 1, r] = up
            dt[t + 1, q] = down

    def come(n):
        with jax.named_scope("arrive_py"):
            for a in (-1, 1):
                if n == 0:
                    for b in (-1, 1):
                        arrive(a, b)
                arrive(a, 0, n)
        with jax.named_scope("outer"):
            for k in DIAGONALS[n]:
                outer(k)

    come(0)
    with jax.named_scope("gather"):
        guess = lax.fori_loop(0, far // 4, lambda i, v: v + sum(dt[STEPS, 2 * STEPS + 4 * i + n, block] for n in range(4)), zero) * (1.0 / far)

        def gather(lines, totals):
            for line in lines:
                moved = line - guess
                totals = (totals[0] + moved, totals[1] + moved * moved)
            return totals

        totals = lax.fori_loop(0, far // 2, lambda i, t: gather([dt[STEPS, 2 * STEPS + 2 * i + n, block] for n in range(2)], t), (zero, zero))

    come(1)
    come(2)
    with jax.named_scope("part"):
        totals = gather([dt[STEPS, r, block] for n in range(STEPS) for r in (TOP + n, TOP + ROWS - 1 - n)], totals)
        offset = totals[0] * (1.0 / ROWS)
        part[0] = guess + offset
        part[1] = totals[1] - totals[0] * offset

    def start(mine, got, count, phase, targets):
        along_x = phase in (0, 2)
        base, here = (0 if phase in (0, 3) else count - 1), (x if along_x else z)
        for target in targets:
            @pl.when(here != target)
            def _():
                at = base + lax.rem(target - here + count, count) - 1
                to = z * XS + target if along_x else target * XS + x
                pltpu.make_async_remote_copy(mine, got.at[at], ts_sem.at[phase], tr_sem.at[phase], device_id={"py": to, "px": px}, device_id_type=MESH).start()

    def done(got, count, phase, sems):
        base = 0 if phase in (0, 3) else count - 1
        cells = got.at[pl.ds(base, count - 1)]
        pltpu.make_async_copy(cells, cells, sems.at[phase]).wait()

    def collect(mine, got, count, phase, each):
        done(got, count, phase, tr_sem)
        base = 0 if phase in (0, 3) else count - 1
        return merged(*([mine[s]] + [got[base + k, s] for k in range(count - 1)] for s in (0, 1)), each)

    halves = [part.at[:, pl.ds(h * HALF, HALF)] for h in (0, 1)]
    cells = float(ROWS)
    start(halves[0], xin, XS, 0, X_ORDER)
    for n in range(1, rounds):
        with jax.named_scope("token"):
            pl.semaphore_wait(token.at[n], 2)
        if n + 1 < rounds:
            tell(n + 1, 2 ** (n + 1))
    start(halves[1], zin, zs, 1, range(zs))

    @pl.loop(0, ROWS)
    def _(i):
        e_out[i] = dt[STEPS, TOP + i, block]

    for a, b, n in beside_sends + corner_sends + near_sends + far_sends:
        @pl.when(there(a, b))
        def _():
            all_of(a, b, n, hs_sem)

    with jax.named_scope("xa"):
        mid_part[0, 0], mid_part[0, 1] = collect(halves[0], xin, XS, 0, cells)
    early = z < zs // 2
    start(mid_part.at[0], zin, zs, 3, range(zs // 2))

    @pl.when(jnp.logical_not(early))
    def _():
        start(mid_part.at[0], zin, zs, 3, range(zs // 2, zs))

    with jax.named_scope("zb"):
        mid_part[1, 0], mid_part[1, 1] = collect(halves[1], zin, zs, 1, cells)
    start(mid_part.at[1], xin, XS, 2, X_ORDER)

    @pl.when(early)
    def _():
        start(mid_part.at[0], zin, zs, 3, range(zs // 2, zs))

    with jax.named_scope("za"):
        mean_a, spread_a = collect(mid_part.at[0], zin, zs, 3, cells * XS)
        stats[0, :HALF] = mean_a
        stats[1, :HALF] = lax.rsqrt(spread_a * (1.0 / (ROWS * npy)) + EPS)
    with jax.named_scope("xb"):
        mean_b, spread_b = collect(mid_part.at[1], xin, XS, 2, cells * zs)
        stats[0, HALF:] = mean_b
        stats[1, HALF:] = lax.rsqrt(spread_b * (1.0 / (ROWS * npy)) + EPS)
    for got, count, phase in ((xin, XS, 0), (zin, zs, 1), (xin, XS, 2), (zin, zs, 3)):
        done(got, count, phase, ts_sem)


def finish(end, stats, a_out, e_out, held, sem):
    whole = pltpu.make_async_copy(end, e_out, sem.at[0])
    whole.start()
    mean, scale = stats[0], stats[1]
    quarter = ROWS // 4
    copies = []
    for q in range(4):
        @pl.loop(q * quarter, (q + 1) * quarter)
        def _(i):
            held[i] = (end[i] - mean) * scale

        rows = pl.ds(q * quarter, quarter)
        copies.append(pltpu.make_async_copy(held.at[rows], a_out.at[rows], sem.at[1 + q]))
        copies[-1].start()
    whole.wait()
    for copy in copies:
        copy.wait()


def solution(mesh):
    npy, npx = mesh.shape["py"], mesh.shape["px"]
    zs = npy // XS

    def per_device(density, conductance, source):
        shape = jax.ShapeDtypeStruct((ROWS, COLS, LEV), jnp.float32)
        f32 = jnp.float32
        dma = pltpu.SemaphoreType.DMA
        end, stats = pl.pallas_call(
            functools.partial(kernel, npy, npx),
            name="diffuse",
            out_shape=(pltpu.VMEM((ROWS, COLS, LEV), f32), pltpu.VMEM((2, COLS, LEV), f32)),
            in_specs=[pl.BlockSpec(memory_space=pl.ANY)] * 3,
            out_specs=[pl.BlockSpec(memory_space=pltpu.VMEM)] * 2,
            scratch_shapes=[
                pltpu.VMEM((STEPS + 1, HIGH, WIDE, LEV), f32),
                pltpu.VMEM((2, HIGH, WIDE, LEV), f32),
                pltpu.VMEM((2, LATE, COLS, LEV), f32),
                pltpu.VMEM((2, LATE, COLS, LEV), f32),
                pltpu.VMEM((2, COLS, LEV), f32),
                pltpu.VMEM((2, 2, HALF, LEV), f32),
                pltpu.VMEM((2 * (XS - 1), 2, HALF, LEV), f32),
                pltpu.VMEM((2 * (zs - 1), 2, HALF, LEV), f32),
                dma((2,)), dma((COPIES,)), dma((COPIES,)),
                dma((4,)), dma((4,)), pltpu.SemaphoreType.REGULAR((2,)), pltpu.SemaphoreType.REGULAR,
            ],
            compiler_params=pltpu.CompilerParams(collective_id=0, has_side_effects=True),
        )(density, conductance, source)
        return pl.pallas_call(
            finish,
            name="finish",
            out_shape=(shape, shape),
            in_specs=[pl.BlockSpec(memory_space=pltpu.VMEM)] * 2,
            out_specs=[pl.BlockSpec(memory_space=pl.ANY)] * 2,
            scratch_shapes=[pltpu.VMEM((ROWS, COLS, LEV), f32), dma((5,))],
        )(*(pltpu.with_memory_space_constraint(v, pltpu.VMEM) for v in (end, stats)))

    spec = P("py", "px", None)
    return jax.shard_map(per_device, mesh=mesh, in_specs=(spec,) * 3, out_specs=(spec, spec), check_vma=False)
```
